256 devices in a mesh: frame: 16 (over z, x_lo), row: 16 (over x_hi, y, core).
Axes of the slice: x: 4 (x_hi: 2, x_lo: 2; x = x_hi * 2 + x_lo), y: 4, z: 8, core: 2. Of those that a mesh axis runs over, the one named last changes fastest.
Arguments:
- frames: float32 [64, 512, 2048], P('frame', 'row'), may hold values from -12 to 12
Outputs:
- estimate: float32 [512, 2048], P('row')
The draws below stay inside these ranges and needn't reach their ends.
All inputs are finite; a program needn't handle non-finite values.
Results may differ from the reference program's by a relative error of at most 0.00002.
Values sent between devices are 32-bit elements; how exact they have to be, the bound alone decides.
A program may use at most 64 MiB of HBM per device.

```python
import jax
import jax.numpy as jnp
from jax import lax

FRAMES = 64
ROUNDS = 3
COLS = 2048
HEIGHT = 512


def draw_frames(key, part):
    scene = jax.random.normal(jax.random.fold_in(key, 11), (HEIGHT, COLS), jnp.float32)
    shape = (FRAMES, HEIGHT, COLS)
    ladder = jnp.arange(FRAMES, dtype=jnp.float32) / (FRAMES - 1)
    jitter = jnp.exp(jax.random.uniform(jax.random.fold_in(key, 12), (FRAMES,), jnp.float32, -0.1, 0.1))
    gains = (0.5 + ladder) * jitter
    noise = 0.3 * jax.random.normal(jax.random.fold_in(key, 13), shape, jnp.float32)
    hits = jax.random.uniform(jax.random.fold_in(key, 14), shape, jnp.float32) < 0.06
    spikes = jax.random.uniform(jax.random.fold_in(key, 15), shape, jnp.float32, -4.0, 4.0)
    result = gains[:, None, None] * scene[None] + noise + jnp.where(hits, spikes, 0.0)
    return jnp.clip(result, -12.0, 12.0)


def setup_inputs(seed: int = 0) -> dict:
    key_list = jax.random.split(jax.random.key(seed), 2)
    return {
        "frames": draw_frames(jax.random.fold_in(key_list[1], 71), 0),
    }


GUIDE_EPS = 0.05
CAUCHY_SCALE = 0.5


def box_sum(field):
    height, width = field.shape
    padded = jnp.pad(field, ((4, 4), (4, 4)))
    rows_total = padded[0:height]
    for offset in range(1, 9):
        rows_total = rows_total + padded[offset:offset + height]
    total = rows_total[:, 0:width]
    for offset in range(1, 9):
        total = total + rows_total[:, offset:offset + width]
    return total


def reference(frames):
    counts = box_sum(jnp.ones(frames.shape[1:], jnp.float32))

    def smooth(field):
        return box_sum(field) / counts

    estimate = jnp.sum(frames, axis=0) / FRAMES
    for round_index in range(ROUNDS):
        mean_guide = smooth(estimate)
        variance = smooth(estimate * estimate) - mean_guide * mean_guide

        def accumulate(carry, frame):
            mean_frame = smooth(frame)
            cross = smooth(estimate * frame)
            slope = (cross - mean_guide * mean_frame) / (variance + GUIDE_EPS)
            offset_term = mean_frame - slope * mean_guide
            filtered = smooth(slope) * estimate + smooth(offset_term)
            gap = (filtered - estimate) / CAUCHY_SCALE
            weight = 1.0 / (1.0 + gap * gap)
            return (carry[0] + weight * frame, carry[1] + weight), None

        zeros = jnp.zeros_like(estimate)
        (weighted, total), unused = lax.scan(accumulate, (zeros, zeros), frames)
        estimate = weighted / total
    return estimate
```

```python
import functools

import jax
import jax.numpy as jnp
from jax import lax
from jax.experimental import pallas as pl
from jax.experimental.pallas import tpu as pltpu
from jax.sharding import PartitionSpec as P

FRAMES = 64
ROUNDS = 3
GUIDE_EPS = 0.05
CAUCHY_SCALE = 0.5

LANES = 128
ROWS = 32
WIN = ROWS + 16
PITCH = 56
HALF = 64
PAIR = 16
CHUNK = 8
MESH = pl.DeviceIdType.MESH

WAYS = ((0, -1), (0, 1), (-1, 0), (1, 0), (-1, -1), (-1, 1), (1, -1), (1, 1))


def snake(i):
    z = i // 2
    return z * 2 + (i % 2 + z) % 2


def windows(a, count):
    two = [a[i] + a[i + 1] for i in range(count + 6)]
    four = [two[i] + two[i + 2] for i in range(count + 4)]
    return [(four[i] + four[i + 4]) + a[i + 8] for i in range(count)]


def down_sum(x):
    n = x.shape[0]
    two = x + pltpu.roll(x, n - 1, 0)
    four = two + pltpu.roll(two, n - 2, 0)
    eight = four + pltpu.roll(four, n - 4, 0)
    return eight[: n - 8] + x[8:]


def across_sum(x):
    n = x.shape[1]
    two = x + pltpu.roll(x, n - 1, 1)
    four = two + pltpu.roll(two, n - 2, 1)
    eight = four + pltpu.roll(four, n - 4, 1)
    return eight + pltpu.roll(x, n - 8, 1)


def window_count(place, limit):
    lower = jnp.maximum(place - 4, 0)
    upper = jnp.minimum(place + 4, limit - 1)
    return jnp.maximum(upper - lower + 1, 1).astype(jnp.float32)


def kernel(
    nf, nr, frames, out, recv, flat, tf, rowbox, mean, area, slope, offset, box1, box2,
    table, est, fin, own_sem, a2a_send, a2a_recv, row_send, row_recv, col_send,
    col_recv, est_send, est_recv, fin_send, fin_recv,
):
    per = FRAMES // nf
    f = lax.axis_index("frame")
    r = lax.axis_index("row")
    c = snake(f)
    up, down = r > 0, r < nr - 1
    left, right = c > 0, c < nf - 1
    left_f = snake(jnp.maximum(c - 1, 0))
    right_f = snake(jnp.minimum(c + 1, nf - 1))

    def there(dr, dc):
        ok = None
        for test, step in ((up, dr == -1), (down, dr == 1), (left, dc == -1), (right, dc == 1)):
            if step:
                ok = test if ok is None else jnp.logical_and(ok, test)
        return ok

    def device(dr, dc):
        return {
            "frame": f if dc == 0 else (left_f if dc < 0 else right_f),
            "row": jnp.clip(r + dr, 0, nr - 1),
        }

    own = pltpu.make_async_copy(
        frames.at[:, :, pl.ds(pl.multiple_of(c * LANES, LANES), LANES)],
        recv.at[pl.ds(f * per, per), pl.ds(8, ROWS), :],
        own_sem,
    )
    own.start()

    est[...] = jnp.zeros_like(est)

    @pl.when(jnp.logical_not(up))
    def _():
        recv[:, 0:8, :] = jnp.zeros((FRAMES, 8, LANES), jnp.float32)

    @pl.when(jnp.logical_not(down))
    def _():
        recv[:, 40:48, :] = jnp.zeros((FRAMES, 8, LANES), jnp.float32)

    @pl.when(jnp.logical_not(left))
    def _():
        tf[:, 0:8, :] = jnp.zeros((32, 8, LANES), jnp.float32)

    @pl.when(jnp.logical_not(right))
    def _():
        tf[:, 136:144, :] = jnp.zeros((32, 8, LANES), jnp.float32)

    barrier = pltpu.get_barrier_semaphore()

    @pl.loop(1, nf)
    def _(s):
        pl.semaphore_signal(
            barrier, inc=1, device_id={"frame": (f + s) % nf, "row": r}, device_id_type=MESH
        )

    others = jnp.int32(nf - 1)
    for dr, dc in WAYS:
        if dr == 0:
            continue

        @pl.when(there(dr, dc))
        def _(dr=dr, dc=dc):
            pl.semaphore_signal(barrier, inc=1, device_id=device(dr, dc), device_id_type=MESH)

        others = others + there(dr, dc).astype(jnp.int32)
    pl.semaphore_wait(barrier, others)

    def block(k, peer, to):
        return pltpu.make_async_remote_copy(
            src_ref=frames.at[
                :, pl.ds(k * CHUNK, CHUNK), pl.ds(pl.multiple_of(snake(to) * LANES, LANES), LANES)
            ],
            dst_ref=recv.at[pl.ds(peer * per, per), pl.ds(8 + k * CHUNK, CHUNK), :],
            send_sem=a2a_send.at[k, to],
            recv_sem=a2a_recv.at[k, peer],
            device_id={"frame": to, "row": r},
            device_id_type=MESH,
        )

    def step_of(s):
        d = (s + 1) // 2
        return jnp.where(s % 2 == 1, d, nf - d)

    order = (0, 3, 1, 2)
    for k in order:

        @pl.loop(1, nf)
        def _(s, k=k):
            block(k, f, (f + step_of(s)) % nf).start()

    def arrived(k):
        @pl.loop(1, nf)
        def _(s):
            peer = (f + s) % nf
            block(k, peer, peer).wait_recv()

    def edge(dr):
        at, to = (8, 40) if dr < 0 else (32, 0)
        i = 0 if dr < 0 else 1
        return pltpu.make_async_remote_copy(
            src_ref=recv.at[:, pl.ds(at, 8), :],
            dst_ref=recv.at[:, pl.ds(to, 8), :],
            send_sem=row_send.at[i],
            recv_sem=row_recv.at[i],
            device_id=device(dr, 0),
            device_id_type=MESH,
        )

    lane = lax.broadcasted_iota(jnp.int32, (8, LANES), 1)
    second = jnp.where(lane >= HALF, PAIR, 0)
    height, width = nr * ROWS, nf * LANES
    place_r = r * ROWS - 4 + lax.broadcasted_iota(jnp.int32, (40, 2 * LANES), 0)
    place_c = c * LANES - 4 + lax.broadcasted_iota(jnp.int32, (40, 2 * LANES), 1)
    cells = window_count(place_r, height) * window_count(place_c, width)
    inside = jnp.where(
        (place_r >= 0) & (place_r < height) & (place_c >= 0) & (place_c < width), 1.0, 0.0
    )
    share = 1.0 / cells

    def keep(top, mid, low):
        both = jnp.concatenate([top, mid, low], axis=0)
        table[0:LANES, :] = both[:, 0:LANES].T
        table[LANES : LANES + 16, :] = both[:, LANES : 2 * LANES].T[0:16]

    def spread(x, row):
        idx = jnp.broadcast_to((second + row)[0:1], x.shape)
        return jnp.take_along_axis(x, idx, axis=1, mode="promise_in_bounds")

    zeros48 = jnp.zeros((WIN, 2 * LANES), jnp.float32)
    keep(zeros48, share * inside, share)

    @pl.loop(0, 24)
    def _(i):
        area[i] = spread(table[0:136, :], 48 + i)

    own.wait()
    arrived(0)

    @pl.when(up)
    def _():
        edge(-1).start()

    arrived(3)

    @pl.when(down)
    def _():
        edge(1).start()

    def lay(at):
        @pl.loop(0, FRAMES)
        def _(p):
            flat[pl.ds(pl.multiple_of(p * PITCH + at, 8), 8), :] = recv[p, at : at + 8, :]

    def turn(q):
        @pl.loop(0, 8)
        def _(i):
            row = q * 8 + i
            a = flat[pl.ds(row, FRAMES, stride=PITCH), :]
            b = flat[pl.ds(row + PAIR, FRAMES, stride=PITCH), :]
            tf[row, 8:136, :] = jnp.concatenate([a, b], axis=0).T

    def side(q, dc):
        at, to = (8, 136) if dc < 0 else (128, 0)
        i = 0 if dc < 0 else 1
        return pltpu.make_async_remote_copy(
            src_ref=tf.at[pl.ds(q * 8, 8), pl.ds(at, 8), :],
            dst_ref=tf.at[pl.ds(q * 8, 8), pl.ds(to, 8), :],
            send_sem=col_send.at[i, q],
            recv_sem=col_recv.at[i, q],
            device_id=device(0, dc),
            device_id_type=MESH,
        )

    def turned(q):
        turn(q)
        for dc in (-1, 1):

            @pl.when(there(0, dc))
            def _(dc=dc):
                side(q, dc).start()

    lay(8)
    lay(32)
    arrived(1)
    lay(16)
    turned(2)

    @pl.when(up)
    def _():
        edge(1).wait_recv()

    lay(0)
    turned(0)
    arrived(2)
    lay(24)
    turned(1)

    @pl.when(down)
    def _():
        edge(-1).wait_recv()

    lay(40)
    turned(3)

    def part(e, way):
        dr, dc = WAYS[way]
        at, size, to = {0: (8, ROWS, 8), -1: (8, 8, 40), 1: (32, 8, 0)}[dr]
        return pltpu.make_async_remote_copy(
            src_ref=est.at[e, 1, pl.ds(at, size), :],
            dst_ref=est.at[e, 1 - dc, pl.ds(to, size), :],
            send_sem=est_send.at[e, way],
            recv_sem=est_recv.at[e, way],
            device_id=device(dr, dc),
            device_id_type=MESH,
        )

    def give(e):
        for way, (dr, dc) in enumerate(WAYS):

            @pl.when(there(dr, dc))
            def _(way=way):
                part(e, way).start()

    def take(e):
        for way, (dr, dc) in enumerate(WAYS):

            @pl.when(there(-dr, -dc))
            def _(way=way):
                part(e, way).wait_recv()

    total = lax.fori_loop(
        0, FRAMES, lambda p, t: t + recv[p, 8:40, :], jnp.zeros((ROWS, LANES), jnp.float32)
    )
    est[0, 1, 8:40, :] = total / FRAMES
    give(0)

    for dc in (-1, 1):

        @pl.when(there(0, -dc))
        def _(dc=dc):
            for q in range(4):
                side(q, dc).wait_recv()

    @pl.loop(0, 18)
    def _(j):
        at = pl.ds(pl.multiple_of(j * 8, 8), 8)
        for i, s in enumerate(windows([tf[i, at, :] for i in range(32)], 24)):
            rowbox[i, at, :] = s

    @pl.loop(0, 24)
    def _(i):
        mean[i] = down_sum(rowbox[i]) * area[i]

    for e in range(ROUNDS):
        take(e)
        near = jnp.concatenate([est[e, 0], est[e, 1], est[e, 2]], axis=1)
        guide = pltpu.roll(near, 3 * LANES - 120, 1)[:, 0 : 2 * LANES]

        def smooth(x):
            x = across_sum(x)
            two = x[0:47] + x[1:48]
            four = two[0:45] + two[2:47]
            return (four[0:40] + four[4:44] + x[8:48]) / cells

        mean_guide = smooth(guide)
        variance = smooth(guide * guide) - mean_guide * mean_guide
        keep(guide, mean_guide, inside / (variance + GUIDE_EPS))

        @pl.loop(0, 18)
        def _(j):
            at = pl.ds(pl.multiple_of(j * 8, 8), 8)
            t = table[at, :]
            products = [tf[i, at, :] * spread(t, i) for i in range(32)]
            for i, s in enumerate(windows(products, 24)):
                rowbox[i, at, :] = s

        @pl.loop(0, 24)
        def _(i):
            t = table[0:136, :]
            guided = spread(t, 48 + i)
            m = mean[i]
            sl = (down_sum(rowbox[i]) * area[i] - guided * m) * spread(t, 88 + i)
            slope[i] = sl
            offset[i] = m - sl * guided

        @pl.loop(0, 17)
        def _(j):
            at = pl.ds(pl.multiple_of(j * 8, 8), 8)
            for src, dst in ((slope, box1), (offset, box2)):
                for i, s in enumerate(windows([src[i, at, :] for i in range(24)], 16)):
                    dst[i, at, :] = s

        wide = lax.broadcasted_iota(jnp.int32, (LANES, LANES), 1)
        low = wide < HALF

        def weigh(i, acc):
            center = spread(table[8:136, :], 8 + i)
            filtered = (down_sum(box1[i]) * center + down_sum(box2[i])) * area[i + 4, 4:132, :]
            gap = (filtered - center) * (1.0 / CAUCHY_SCALE)
            weight = 1.0 / (1.0 + gap * gap)
            for x, at in ((weight, 0), (weight * tf[i + 8, 8:136, :], 16)):
                a = jnp.sum(jnp.where(low, x, 0.0), axis=1, keepdims=True)
                b = jnp.sum(jnp.where(low, 0.0, x), axis=1, keepdims=True)
                acc = jnp.where(wide == at + i, a, acc)
                acc = jnp.where(wide == HALF + at + i, b, acc)
            return acc

        acc = lax.fori_loop(0, PAIR, weigh, jnp.zeros((LANES, LANES), jnp.float32)).T
        new = jnp.concatenate(
            [acc[16:32] / acc[0:16], acc[80:96] / acc[64:80]], axis=0
        )
        if e < ROUNDS - 1:
            est[e + 1, 1, 8:40, :] = new
            give(e + 1)
        else:
            fin[...] = new

    def final(of, to):
        return pltpu.make_async_remote_copy(
            src_ref=fin,
            dst_ref=out.at[:, pl.ds(pl.multiple_of(snake(of) * LANES, LANES), LANES)],
            send_sem=fin_send.at[to],
            recv_sem=fin_recv.at[of],
            device_id={"frame": to, "row": r},
            device_id_type=MESH,
        )

    @pl.loop(1, nf)
    def _(s):
        final(f, (f + step_of(s)) % nf).start()

    mine = pltpu.make_async_copy(
        fin, out.at[:, pl.ds(pl.multiple_of(c * LANES, LANES), LANES)], own_sem
    )
    mine.start()

    for k in order:

        @pl.loop(1, nf)
        def _(s, k=k):
            block(k, f, (f + s) % nf).wait_send()

    for dr in (-1, 1):

        @pl.when(there(dr, 0))
        def _(dr=dr):
            edge(dr).wait_send()

    for dc in (-1, 1):

        @pl.when(there(0, dc))
        def _(dc=dc):
            for q in range(4):
                side(q, dc).wait_send()

    for e in range(ROUNDS):
        for way, (dr, dc) in enumerate(WAYS):

            @pl.when(there(dr, dc))
            def _(e=e, way=way):
                part(e, way).wait_send()

    @pl.loop(1, nf)
    def _(s):
        peer = (f + s) % nf
        final(peer, peer).wait_recv()
        final(f, peer).wait_send()

    mine.wait()


def merge(nf, nr, frames):
    f32 = jnp.float32
    dma = pltpu.SemaphoreType.DMA
    return pl.pallas_call(
        functools.partial(kernel, nf, nr),
        out_shape=jax.ShapeDtypeStruct((ROWS, nf * LANES), f32),
        in_specs=[pl.BlockSpec(memory_space=pl.ANY)],
        out_specs=pl.BlockSpec(memory_space=pl.ANY),
        scratch_shapes=[
            pltpu.VMEM((FRAMES, WIN, LANES), f32),
            pltpu.VMEM((FRAMES * PITCH, LANES), f32),
            pltpu.VMEM((32, 144, LANES), f32),
            pltpu.VMEM((24, 144, LANES), f32),
            pltpu.VMEM((24, 136, LANES), f32),
            pltpu.VMEM((24, 136, LANES), f32),
            pltpu.VMEM((24, 136, LANES), f32),
            pltpu.VMEM((24, 136, LANES), f32),
            pltpu.VMEM((16, 136, LANES), f32),
            pltpu.VMEM((16, 136, LANES), f32),
            pltpu.VMEM((144, LANES), f32),
            pltpu.VMEM((ROUNDS, 3, WIN, LANES), f32),
            pltpu.VMEM((ROWS, LANES), f32),
            dma,
            dma((4, nf)),
            dma((4, nf)),
            dma((2,)),
            dma((2,)),
            dma((2, 4)),
            dma((2, 4)),
            dma((ROUNDS, 8)),
            dma((ROUNDS, 8)),
            dma((nf,)),
            dma((nf,)),
        ],
        compiler_params=pltpu.CompilerParams(collective_id=0, has_side_effects=True),
        name="merge",
    )(frames)


def solution(mesh):
    return jax.shard_map(
        functools.partial(merge, mesh.shape["frame"], mesh.shape["row"]),
        mesh=mesh,
        in_specs=(P("frame", "row", None),),
        out_specs=P("row", None),
        check_vma=False,
    )
```

```python
import functools

import jax
import jax.numpy as jnp
from jax import lax
from jax.experimental import pallas as pl
from jax.experimental.pallas import tpu as pltpu
from jax.sharding import PartitionSpec as P

FRAMES = 64
ROUNDS = 3
GUIDE_EPS = 0.05
CAUCHY_SCALE = 0.5

LANES = 128
ROWS = 32
WIN = ROWS + 16
PITCH = 56
HALF = 64
PAIR = 16
CHUNK = 8
MESH = pl.DeviceIdType.MESH

WAYS = ((0, -1), (0, 1), (-1, 0), (1, 0), (-1, -1), (-1, 1), (1, -1), (1, 1))


def snake(i):
    z = i // 2
    return z * 2 + (i % 2 + z) % 2


def windows(a, count):
    two = [a[i] + a[i + 1] for i in range(count + 6)]
    four = [two[i] + two[i + 2] for i in range(count + 4)]
    return [(four[i] + four[i + 4]) + a[i + 8] for i in range(count)]


def down_sum(x):
    n = x.shape[0]
    two = x + pltpu.roll(x, n - 1, 0)
    four = two + pltpu.roll(two, n - 2, 0)
    eight = four + pltpu.roll(four, n - 4, 0)
    return eight[: n - 8] + x[8:]


def across_sum(x):
    n = x.shape[1]
    two = x + pltpu.roll(x, n - 1, 1)
    four = two + pltpu.roll(two, n - 2, 1)
    eight = four + pltpu.roll(four, n - 4, 1)
    return eight + pltpu.roll(x, n - 8, 1)


def thirds(x):
    high = x.astype(jnp.bfloat16)
    rest = x - high.astype(jnp.float32)
    mid = rest.astype(jnp.bfloat16)
    return high, mid, (rest - mid.astype(jnp.float32)).astype(jnp.bfloat16)


def stacked(*arrays):
    rows = [t.astype(jnp.float32) for a in arrays for t in thirds(a)]
    spare = 256 - sum(t.shape[0] for t in rows)
    rows.append(jnp.zeros((spare, rows[0].shape[1]), jnp.float32))
    return jnp.concatenate(rows, axis=0).astype(jnp.bfloat16).T[0:144]


def window_count(place, limit):
    lower = jnp.maximum(place - 4, 0)
    upper = jnp.minimum(place + 4, limit - 1)
    return jnp.maximum(upper - lower + 1, 1).astype(jnp.float32)


def kernel(
    nf, nr, frames, out, recv, flat, tf, rowbox, mean, area, slope, offset, box1, box2,
    table, gb, guide_t, stat_t, pick_g, pick_s, pick_w, est, fin, own_sem, a2a_send, a2a_recv, row_send, row_recv, col_send,
    col_recv, est_send, est_recv, fin_send, fin_recv,
):
    per = FRAMES // nf
    f = lax.axis_index("frame")
    r = lax.axis_index("row")
    c = snake(f)
    up, down = r > 0, r < nr - 1
    left, right = c > 0, c < nf - 1
    left_f = snake(jnp.maximum(c - 1, 0))
    right_f = snake(jnp.minimum(c + 1, nf - 1))

    def there(dr, dc):
        ok = None
        for test, step in ((up, dr == -1), (down, dr == 1), (left, dc == -1), (right, dc == 1)):
            if step:
                ok = test if ok is None else jnp.logical_and(ok, test)
        return ok

    def device(dr, dc):
        return {
            "frame": f if dc == 0 else (left_f if dc < 0 else right_f),
            "row": jnp.clip(r + dr, 0, nr - 1),
        }

    own = pltpu.make_async_copy(
        frames.at[:, :, pl.ds(pl.multiple_of(c * LANES, LANES), LANES)],
        recv.at[pl.ds(f * per, per), pl.ds(8, ROWS), :],
        own_sem,
    )
    own.start()

    est[...] = jnp.zeros_like(est)

    @pl.when(jnp.logical_not(up))
    def _():
        recv[:, 0:8, :] = jnp.zeros((FRAMES, 8, LANES), jnp.float32)

    @pl.when(jnp.logical_not(down))
    def _():
        recv[:, 40:48, :] = jnp.zeros((FRAMES, 8, LANES), jnp.float32)

    @pl.when(jnp.logical_not(left))
    def _():
        tf[:, 0:8, :] = jnp.zeros((32, 8, LANES), jnp.float32)

    @pl.when(jnp.logical_not(right))
    def _():
        tf[:, 136:144, :] = jnp.zeros((32, 8, LANES), jnp.float32)

    barrier = pltpu.get_barrier_semaphore()

    @pl.loop(1, nf)
    def _(s):
        pl.semaphore_signal(
            barrier, inc=1, device_id={"frame": (f + s) % nf, "row": r}, device_id_type=MESH
        )

    others = jnp.int32(nf - 1)
    for dr, dc in WAYS:
        if dr == 0:
            continue

        @pl.when(there(dr, dc))
        def _(dr=dr, dc=dc):
            pl.semaphore_signal(barrier, inc=1, device_id=device(dr, dc), device_id_type=MESH)

        others = others + there(dr, dc).astype(jnp.int32)
    pl.semaphore_wait(barrier, others)

    def block(k, peer, to):
        return pltpu.make_async_remote_copy(
            src_ref=frames.at[
                :, pl.ds(k * CHUNK, CHUNK), pl.ds(pl.multiple_of(snake(to) * LANES, LANES), LANES)
            ],
            dst_ref=recv.at[pl.ds(peer * per, per), pl.ds(8 + k * CHUNK, CHUNK), :],
            send_sem=a2a_send.at[k, to],
            recv_sem=a2a_recv.at[k, peer],
            device_id={"frame": to, "row": r},
            device_id_type=MESH,
        )

    def step_of(s):
        d = (s + 1) // 2
        return jnp.where(s % 2 == 1, d, nf - d)

    order = (0, 3, 1, 2)
    for k in order:

        @pl.loop(1, nf)
        def _(s, k=k):
            block(k, f, (f + step_of(s)) % nf).start()

    def arrived(k):
        @pl.loop(1, nf)
        def _(s):
            peer = (f + s) % nf
            block(k, peer, peer).wait_recv()

    def edge(dr):
        at, to = (8, 40) if dr < 0 else (32, 0)
        i = 0 if dr < 0 else 1
        return pltpu.make_async_remote_copy(
            src_ref=recv.at[:, pl.ds(at, 8), :],
            dst_ref=recv.at[:, pl.ds(to, 8), :],
            send_sem=row_send.at[i],
            recv_sem=row_recv.at[i],
            device_id=device(dr, 0),
            device_id_type=MESH,
        )

    lane = lax.broadcasted_iota(jnp.int32, (8, LANES), 1)
    second = jnp.where(lane >= HALF, PAIR, 0)
    height, width = nr * ROWS, nf * LANES
    place_r = r * ROWS - 4 + lax.broadcasted_iota(jnp.int32, (40, 2 * LANES), 0)
    place_c = c * LANES - 4 + lax.broadcasted_iota(jnp.int32, (40, 2 * LANES), 1)
    cells = window_count(place_r, height) * window_count(place_c, width)
    inside = jnp.where(
        (place_r >= 0) & (place_r < height) & (place_c >= 0) & (place_c < width), 1.0, 0.0
    )
    share = 1.0 / cells

    def keep(top, mid, low):
        both = jnp.concatenate([top, mid, low], axis=0)
        table[0:LANES, :] = both[:, 0:LANES].T
        table[LANES : LANES + 16, :] = both[:, LANES : 2 * LANES].T[0:16]

    def spread(x, row):
        idx = jnp.broadcast_to((second + row)[0:1], x.shape)
        return jnp.take_along_axis(x, idx, axis=1, mode="promise_in_bounds")

    zeros48 = jnp.zeros((WIN, 2 * LANES), jnp.float32)
    keep(zeros48, share * inside, share)

    @pl.loop(0, 24)
    def _(i):
        area[i] = spread(table[0:136, :], 48 + i)

    k = lax.broadcasted_iota(jnp.int32, (256, 256), 0)
    n = lax.broadcasted_iota(jnp.int32, (256, 256), 1)
    side_n, half_n = n // LANES, jnp.where(n % LANES >= HALF, PAIR, 0)
    row_g = jnp.where(k < 144, k % 48, 255) - half_n - side_n
    row_s = jnp.where(k // 120 == side_n, k % 40, 255) - half_n

    @pl.loop(0, 16)
    def _(q):
        pick_g[q] = jnp.where(row_g == 2 * q, 1.0, 0.0).astype(jnp.bfloat16)

    @pl.loop(0, 24)
    def _(i):
        pick_s[i] = jnp.where(row_s == i, 1.0, 0.0).astype(jnp.bfloat16)

    k = lax.broadcasted_iota(jnp.int32, (384, LANES), 0) % LANES
    n = lax.broadcasted_iota(jnp.int32, (384, LANES), 1)
    row_w = n - jnp.where(k >= HALF, HALF, 0) - jnp.where(k % HALF >= 32, 0, 16)

    @pl.loop(0, PAIR)
    def _(i):
        pick_w[i] = jnp.where(row_w == i, 1.0, 0.0).astype(jnp.bfloat16)

    own.wait()
    arrived(0)

    @pl.when(up)
    def _():
        edge(-1).start()

    arrived(3)

    @pl.when(down)
    def _():
        edge(1).start()

    def lay(at):
        @pl.loop(0, FRAMES, unroll=8)
        def _(p):
            flat[pl.ds(pl.multiple_of(p * PITCH + at, 8), 8), :] = recv[p, at : at + 8, :]

    def turn(q):
        @pl.loop(0, 8, unroll=8)
        def _(i):
            row = q * 8 + i
            a = flat[pl.ds(row, FRAMES, stride=PITCH), :]
            b = flat[pl.ds(row + PAIR, FRAMES, stride=PITCH), :]
            tf[row, 8:136, :] = jnp.concatenate([a, b], axis=0).T

    def side(q, dc):
        at, to = (8, 136) if dc < 0 else (128, 0)
        i = 0 if dc < 0 else 1
        return pltpu.make_async_remote_copy(
            src_ref=tf.at[pl.ds(q * 8, 8), pl.ds(at, 8), :],
            dst_ref=tf.at[pl.ds(q * 8, 8), pl.ds(to, 8), :],
            send_sem=col_send.at[i, q],
            recv_sem=col_recv.at[i, q],
            device_id=device(0, dc),
            device_id_type=MESH,
        )

    def turned(q):
        turn(q)
        for dc in (-1, 1):

            @pl.when(there(0, dc))
            def _(dc=dc):
                side(q, dc).start()

    lay(8)
    lay(32)
    def part(e, way):
        dr, dc = WAYS[way]
        at, size, to = {0: (8, ROWS, 8), -1: (8, 8, 40), 1: (32, 8, 0)}[dr]
        return pltpu.make_async_remote_copy(
            src_ref=est.at[e, 1, pl.ds(at, size), :],
            dst_ref=est.at[e, 1 - dc, pl.ds(to, size), :],
            send_sem=est_send.at[e, way],
            recv_sem=est_recv.at[e, way],
            device_id=device(dr, dc),
            device_id_type=MESH,
        )

    def give(e):
        for way, (dr, dc) in enumerate(WAYS):

            @pl.when(there(dr, dc))
            def _(way=way):
                part(e, way).start()

    def take(e):
        for way, (dr, dc) in enumerate(WAYS):

            @pl.when(there(-dr, -dc))
            def _(way=way):
                part(e, way).wait_recv()

    def start(at):
        total = lax.fori_loop(
            0, FRAMES, lambda p, t: t + recv[p, at : at + 8, :], jnp.zeros((8, LANES), jnp.float32),
            unroll=16,
        )
        est[0, 1, at : at + 8, :] = total / FRAMES

    start(8)
    start(32)
    arrived(1)
    start(16)
    lay(16)
    turned(2)

    @pl.when(up)
    def _():
        edge(1).wait_recv()

    lay(0)
    turned(0)
    arrived(2)
    start(24)
    give(0)
    lay(24)
    turned(1)

    @pl.when(down)
    def _():
        edge(-1).wait_recv()

    lay(40)
    turned(3)

    for dc in (-1, 1):

        @pl.when(there(0, -dc))
        def _(dc=dc):
            for q in range(4):
                side(q, dc).wait_recv()

    @pl.loop(0, 18)
    def _(j):
        at = pl.ds(pl.multiple_of(j * 8, 8), 8)
        for i, s in enumerate(windows([tf[i, at, :] for i in range(32)], 24)):
            rowbox[i, at, :] = s

    @pl.loop(0, 24, unroll=4)
    def _(i):
        mean[i] = down_sum(rowbox[i]) * area[i]

    for e in range(ROUNDS):
        take(e)
        near = jnp.concatenate([est[e, 0], est[e, 1], est[e, 2]], axis=1)
        guide = pltpu.roll(near, 3 * LANES - 120, 1)[:, 0 : 2 * LANES]

        def smooth(x):
            x = across_sum(x)
            two = x[0:47] + x[1:48]
            four = two[0:45] + two[2:47]
            return (four[0:40] + four[4:44] + x[8:48]) / cells

        mean_guide = smooth(guide)
        variance = smooth(guide * guide) - mean_guide * mean_guide
        guide_t[...] = stacked(guide)
        stat_t[...] = stacked(mean_guide, inside / (variance + GUIDE_EPS))

        @pl.loop(0, 16, unroll=16)
        def _(q):
            two = jnp.dot(guide_t[...], pick_g[q], preferred_element_type=jnp.float32)
            gb[2 * q] = two[:, 0:LANES]
            gb[2 * q + 1] = two[:, LANES:]

        @pl.loop(0, 18, unroll=2)
        def _(j):
            at = pl.ds(pl.multiple_of(j * 8, 8), 8)
            products = [tf[i, at, :] * gb[i, at, :] for i in range(32)]
            for i, s in enumerate(windows(products, 24)):
                rowbox[i, at, :] = s

        @pl.loop(0, 24, unroll=8)
        def _(i):
            both = jnp.dot(stat_t[...], pick_s[i], preferred_element_type=jnp.float32)
            guided = both[0:136, 0:LANES]
            m = mean[i]
            sl = (down_sum(rowbox[i]) * area[i] - guided * m) * both[0:136, LANES:]
            slope[i] = sl
            offset[i] = m - sl * guided

        @pl.loop(0, 17)
        def _(j):
            at = pl.ds(pl.multiple_of(j * 8, 8), 8)
            for src, dst in ((slope, box1), (offset, box2)):
                for i, s in enumerate(windows([src[i, at, :] for i in range(24)], 16)):
                    dst[i, at, :] = s

        wide = lax.broadcasted_iota(jnp.int32, (LANES, LANES), 1)
        late = wide % HALF >= 32

        def weigh(i, acc):
            center = gb[8 + i, 8:136, :]
            filtered = (down_sum(box1[i]) * center + down_sum(box2[i])) * area[i + 4, 4:132, :]
            gap = (filtered - center) * (1.0 / CAUCHY_SCALE)
            w = 1.0 / (1.0 + gap * gap)
            wp = w * tf[i + 8, 8:136, :]
            part_sums = jnp.where(late, w + pltpu.roll(w, 32, 1), wp + pltpu.roll(wp, 96, 1))
            return acc + jnp.dot(
                jnp.concatenate(thirds(part_sums), axis=1),
                pick_w[i],
                preferred_element_type=jnp.float32,
            )

        acc = lax.fori_loop(0, PAIR, weigh, jnp.zeros((LANES, LANES), jnp.float32), unroll=8).T
        new = jnp.concatenate(
            [acc[16:32] / acc[0:16], acc[80:96] / acc[64:80]], axis=0
        )
        if e < ROUNDS - 1:
            est[e + 1, 1, 8:40, :] = new
            give(e + 1)
        else:
            fin[...] = new

    def final(of, to):
        return pltpu.make_async_remote_copy(
            src_ref=fin,
            dst_ref=out.at[:, pl.ds(pl.multiple_of(snake(of) * LANES, LANES), LANES)],
            send_sem=fin_send.at[to],
            recv_sem=fin_recv.at[of],
            device_id={"frame": to, "row": r},
            device_id_type=MESH,
        )

    @pl.loop(1, nf)
    def _(s):
        final(f, (f + step_of(s)) % nf).start()

    mine = pltpu.make_async_copy(
        fin, out.at[:, pl.ds(pl.multiple_of(c * LANES, LANES), LANES)], own_sem
    )
    mine.start()

    for k in order:

        @pl.loop(1, nf)
        def _(s, k=k):
            block(k, f, (f + s) % nf).wait_send()

    for dr in (-1, 1):

        @pl.when(there(dr, 0))
        def _(dr=dr):
            edge(dr).wait_send()

    for dc in (-1, 1):

        @pl.when(there(0, dc))
        def _(dc=dc):
            for q in range(4):
                side(q, dc).wait_send()

    for e in range(ROUNDS):
        for way, (dr, dc) in enumerate(WAYS):

            @pl.when(there(dr, dc))
            def _(e=e, way=way):
                part(e, way).wait_send()

    @pl.loop(1, nf)
    def _(s):
        peer = (f + s) % nf
        final(peer, peer).wait_recv()
        final(f, peer).wait_send()

    mine.wait()


def merge(nf, nr, frames):
    f32 = jnp.float32
    dma = pltpu.SemaphoreType.DMA
    return pl.pallas_call(
        functools.partial(kernel, nf, nr),
        out_shape=jax.ShapeDtypeStruct((ROWS, nf * LANES), f32),
        in_specs=[pl.BlockSpec(memory_space=pl.ANY)],
        out_specs=pl.BlockSpec(memory_space=pl.ANY),
        scratch_shapes=[
            pltpu.VMEM((FRAMES, WIN, LANES), f32),
            pltpu.VMEM((FRAMES * PITCH, LANES), f32),
            pltpu.VMEM((32, 144, LANES), f32),
            pltpu.VMEM((24, 144, LANES), f32),
            pltpu.VMEM((24, 136, LANES), f32),
            pltpu.VMEM((24, 136, LANES), f32),
            pltpu.VMEM((24, 136, LANES), f32),
            pltpu.VMEM((24, 136, LANES), f32),
            pltpu.VMEM((16, 136, LANES), f32),
            pltpu.VMEM((16, 136, LANES), f32),
            pltpu.VMEM((144, LANES), f32),
            pltpu.VMEM((32, 144, LANES), f32),
            pltpu.VMEM((144, 256), jnp.bfloat16),
            pltpu.VMEM((144, 256), jnp.bfloat16),
            pltpu.VMEM((16, 256, 256), jnp.bfloat16),
            pltpu.VMEM((24, 256, 256), jnp.bfloat16),
            pltpu.VMEM((16, 384, LANES), jnp.bfloat16),
            pltpu.VMEM((ROUNDS, 3, WIN, LANES), f32),
            pltpu.VMEM((ROWS, LANES), f32),
            dma,
            dma((4, nf)),
            dma((4, nf)),
            dma((2,)),
            dma((2,)),
            dma((2, 4)),
            dma((2, 4)),
            dma((ROUNDS, 8)),
            dma((ROUNDS, 8)),
            dma((nf,)),
            dma((nf,)),
        ],
        compiler_params=pltpu.CompilerParams(collective_id=0, has_side_effects=True),
        name="merge",
    )(frames)


def solution(mesh):
    return jax.shard_map(
        functools.partial(merge, mesh.shape["frame"], mesh.shape["row"]),
        mesh=mesh,
        in_specs=(P("frame", "row", None),),
        out_specs=P("row", None),
        check_vma=False,
    )
```

```python
import functools

import jax
import jax.numpy as jnp
from jax import lax
from jax.experimental import pallas as pl
from jax.experimental.pallas import tpu as pltpu
from jax.sharding import PartitionSpec as P

FRAMES = 64
ROUNDS = 3
GUIDE_EPS = 0.05
CAUCHY_SCALE = 0.5

LANES = 128
ROWS = 32
WIN = ROWS + 16
PITCH = 56
HALF = 64
PAIR = 16
CHUNK = 8
MESH = pl.DeviceIdType.MESH

WAYS = ((0, -1), (0, 1), (-1, 0), (1, 0), (-1, -1), (-1, 1), (1, -1), (1, 1))


def snake(i):
    z = i // 2
    return z * 2 + (i % 2 + z) % 2


def windows(a, count):
    two = [a[i] + a[i + 1] for i in range(count + 6)]
    four = [two[i] + two[i + 2] for i in range(count + 4)]
    return [(four[i] + four[i + 4]) + a[i + 8] for i in range(count)]


def down_sum(x):
    n = x.shape[0]
    two = x + pltpu.roll(x, n - 1, 0)
    four = two + pltpu.roll(two, n - 2, 0)
    eight = four + pltpu.roll(four, n - 4, 0)
    return eight[: n - 8] + x[8:]


def across_sum(x):
    n = x.shape[1]
    two = x + pltpu.roll(x, n - 1, 1)
    four = two + pltpu.roll(two, n - 2, 1)
    eight = four + pltpu.roll(four, n - 4, 1)
    return eight + pltpu.roll(x, n - 8, 1)


def thirds(x):
    high = x.astype(jnp.bfloat16)
    rest = x - high.astype(jnp.float32)
    mid = rest.astype(jnp.bfloat16)
    return high, mid, (rest - mid.astype(jnp.float32)).astype(jnp.bfloat16)


def stacked(*arrays):
    rows = [t.astype(jnp.float32) for a in arrays for t in thirds(a)]
    spare = 256 - sum(t.shape[0] for t in rows)
    rows.append(jnp.zeros((spare, rows[0].shape[1]), jnp.float32))
    return jnp.concatenate(rows, axis=0).astype(jnp.bfloat16).T[0:144]


def window_count(place, limit):
    lower = jnp.maximum(place - 4, 0)
    upper = jnp.minimum(place + 4, limit - 1)
    return jnp.maximum(upper - lower + 1, 1).astype(jnp.float32)


def kernel(
    nf, nr, frames, out, recv, flat, tf, rowbox, rowmean, mean, area, slope, offset, box1, box2,
    table, gb, guide_t, stat_t, pick_g, pick_s, pick_w, est, fin, turned_sums, own_sem, a2a_send, a2a_recv, row_send, row_recv, col_send,
    col_recv, est_send, est_recv, fin_send, fin_recv,
):
    per = FRAMES // nf
    f = lax.axis_index("frame")
    r = lax.axis_index("row")
    c = snake(f)
    up, down = r > 0, r < nr - 1
    left, right = c > 0, c < nf - 1
    odd = r % 2 == 1
    first = 8 * (r % 2)
    left_f = snake(jnp.maximum(c - 1, 0))
    right_f = snake(jnp.minimum(c + 1, nf - 1))

    def there(dr, dc):
        ok = None
        for test, step in ((up, dr == -1), (down, dr == 1), (left, dc == -1), (right, dc == 1)):
            if step:
                ok = test if ok is None else jnp.logical_and(ok, test)
        return ok

    def device(dr, dc):
        return {
            "frame": f if dc == 0 else (left_f if dc < 0 else right_f),
            "row": jnp.clip(r + dr, 0, nr - 1),
        }

    own = pltpu.make_async_copy(
        frames.at[:, :, pl.ds(pl.multiple_of(c * LANES, LANES), LANES)],
        recv.at[pl.ds(f * per, per), pl.ds(8, ROWS), :],
        own_sem,
    )
    own.start()

    est[...] = jnp.zeros_like(est)

    @pl.when(jnp.logical_not(up))
    def _():
        recv[:, 0:8, :] = jnp.zeros((FRAMES, 8, LANES), jnp.float32)

    @pl.when(jnp.logical_not(down))
    def _():
        recv[:, 40:48, :] = jnp.zeros((FRAMES, 8, LANES), jnp.float32)

    @pl.when(jnp.logical_not(left))
    def _():
        tf[:, 0:8, :] = jnp.zeros((32, 8, LANES), jnp.float32)

    @pl.when(jnp.logical_not(right))
    def _():
        tf[:, 136:144, :] = jnp.zeros((32, 8, LANES), jnp.float32)

    barrier = pltpu.get_barrier_semaphore()

    @pl.loop(1, nf)
    def _(s):
        pl.semaphore_signal(
            barrier, inc=1, device_id={"frame": (f + s) % nf, "row": r}, device_id_type=MESH
        )

    others = jnp.int32(nf - 1)
    for dr, dc in WAYS:
        if dr == 0:
            continue

        @pl.when(there(dr, dc))
        def _(dr=dr, dc=dc):
            pl.semaphore_signal(barrier, inc=1, device_id=device(dr, dc), device_id_type=MESH)

        others = others + there(dr, dc).astype(jnp.int32)
    pl.semaphore_wait(barrier, others)

    def block(k, peer, to):
        return pltpu.make_async_remote_copy(
            src_ref=frames.at[
                :, pl.ds(k * CHUNK, CHUNK), pl.ds(pl.multiple_of(snake(to) * LANES, LANES), LANES)
            ],
            dst_ref=recv.at[pl.ds(peer * per, per), pl.ds(8 + k * CHUNK, CHUNK), :],
            send_sem=a2a_send.at[k, to],
            recv_sem=a2a_recv.at[k, peer],
            device_id={"frame": to, "row": r},
            device_id_type=MESH,
        )

    def step_of(s):
        d = (s + 1) // 2
        return jnp.where(s % 2 == 1, d, nf - d)

    order = (0, 3, 1, 2)
    for k in order:

        @pl.loop(1, nf)
        def _(s, k=k):
            block(k, f, (f + step_of(s)) % nf).start()

    def arrived(k):
        @pl.loop(1, nf)
        def _(s):
            peer = (f + s) % nf
            block(k, peer, peer).wait_recv()

    def edge(dr):
        at, to = (8, 40) if dr < 0 else (32, 0)
        i = 0 if dr < 0 else 1
        return pltpu.make_async_remote_copy(
            src_ref=recv.at[:, pl.ds(at, 8), :],
            dst_ref=recv.at[:, pl.ds(to, 8), :],
            send_sem=row_send.at[i],
            recv_sem=row_recv.at[i],
            device_id=device(dr, 0),
            device_id_type=MESH,
        )

    lane = lax.broadcasted_iota(jnp.int32, (8, LANES), 1)
    second = jnp.where(lane >= HALF, PAIR, 0)
    height, width = nr * ROWS, nf * LANES
    place_r = r * ROWS - 4 + lax.broadcasted_iota(jnp.int32, (40, 2 * LANES), 0)
    place_c = c * LANES - 4 + lax.broadcasted_iota(jnp.int32, (40, 2 * LANES), 1)
    cells = window_count(place_r, height) * window_count(place_c, width)
    inside = jnp.where(
        (place_r >= 0) & (place_r < height) & (place_c >= 0) & (place_c < width), 1.0, 0.0
    )
    share = 1.0 / cells

    def keep(top, mid, low):
        both = jnp.concatenate([top, mid, low], axis=0)
        table[0:LANES, :] = both[:, 0:LANES].T
        table[LANES : LANES + 16, :] = both[:, LANES : 2 * LANES].T[0:16]

    def spread(x, row):
        idx = jnp.broadcast_to((second + row)[0:1], x.shape)
        return jnp.take_along_axis(x, idx, axis=1, mode="promise_in_bounds")

    zeros48 = jnp.zeros((WIN, 2 * LANES), jnp.float32)
    keep(zeros48, share * inside, share)

    @pl.loop(0, 24)
    def _(i):
        area[i] = spread(table[0:136, :], 48 + i)

    k = lax.broadcasted_iota(jnp.int32, (256, 256), 0)
    n = lax.broadcasted_iota(jnp.int32, (256, 256), 1)
    side_n, half_n = n // LANES, jnp.where(n % LANES >= HALF, PAIR, 0)
    row_g = jnp.where(k < 144, k % 48, 255) - half_n - side_n
    row_s = jnp.where(k // 120 == side_n, k % 40, 255) - half_n

    @pl.loop(0, 16)
    def _(q):
        pick_g[q] = jnp.where(row_g == 2 * q, 1.0, 0.0).astype(jnp.bfloat16)

    @pl.loop(0, 24)
    def _(i):
        pick_s[i] = jnp.where(row_s == i, 1.0, 0.0).astype(jnp.bfloat16)

    k = lax.broadcasted_iota(jnp.int32, (384, LANES), 0) % LANES
    n = lax.broadcasted_iota(jnp.int32, (384, LANES), 1)
    row_w = n - jnp.where(k >= HALF, HALF, 0) - jnp.where(k % HALF >= 32, 0, 16)

    @pl.loop(0, PAIR)
    def _(i):
        pick_w[i] = jnp.where(row_w == i, 1.0, 0.0).astype(jnp.bfloat16)

    own.wait()
    arrived(0)

    @pl.when(up)
    def _():
        edge(-1).start()

    arrived(3)

    @pl.when(down)
    def _():
        edge(1).start()

    def lay(at):
        @pl.loop(0, FRAMES, unroll=8)
        def _(p):
            flat[pl.ds(pl.multiple_of(p * PITCH + at, 8), 8), :] = recv[p, at : at + 8, :]

    def turn(q):
        @pl.loop(0, 8, unroll=8)
        def _(i):
            row = q * 8 + i
            a = flat[pl.ds(row, FRAMES, stride=PITCH), :]
            b = flat[pl.ds(row + PAIR, FRAMES, stride=PITCH), :]
            tf[row, 8:136, :] = jnp.concatenate([a, b], axis=0).T

    def side(q, dc):
        at, to = (8, 136) if dc < 0 else (128, 0)
        i = 0 if dc < 0 else 1
        return pltpu.make_async_remote_copy(
            src_ref=tf.at[pl.ds(q * 8, 8), pl.ds(at, 8), :],
            dst_ref=tf.at[pl.ds(q * 8, 8), pl.ds(to, 8), :],
            send_sem=col_send.at[i, q],
            recv_sem=col_recv.at[i, q],
            device_id=device(0, dc),
            device_id_type=MESH,
        )

    def turned(q):
        turn(q)
        for dc in (-1, 1):

            @pl.when(there(0, dc))
            def _(dc=dc):
                side(q, dc).start()

    lay(8)
    lay(32)
    def part(e, way):
        dr, dc = WAYS[way]
        at, size, to = {0: (8, ROWS, 8), -1: (8, 8, 40), 1: (32, 8, 0)}[dr]
        return pltpu.make_async_remote_copy(
            src_ref=est.at[e, 1, pl.ds(at, size), :],
            dst_ref=est.at[e, 1 - dc, pl.ds(to, size), :],
            send_sem=est_send.at[e, way],
            recv_sem=est_recv.at[e, way],
            device_id=device(dr, dc),
            device_id_type=MESH,
        )

    def give(e, ways):
        for way in ways:

            @pl.when(there(*WAYS[way]))
            def _(way=way):
                part(e, way).start()

    def give_rows(e, late):
        @pl.when(odd != late)
        def _():
            give(e, (3, 6, 7))

        @pl.when(odd == late)
        def _():
            give(e, (2, 4, 5))

    def take(e):
        for way, (dr, dc) in enumerate(WAYS):

            @pl.when(there(-dr, -dc))
            def _(way=way):
                part(e, way).wait_recv()

    def start(at):
        total = lax.fori_loop(
            0, FRAMES, lambda p, t: t + recv[p, at : at + 8, :], jnp.zeros((8, LANES), jnp.float32),
            unroll=16,
        )
        est[0, 1, at : at + 8, :] = total / FRAMES

    start(8)
    start(32)
    give_rows(0, False)
    give_rows(0, True)
    arrived(1)
    start(16)
    lay(16)
    turned(2)

    @pl.when(up)
    def _():
        edge(1).wait_recv()

    lay(0)
    turned(0)
    arrived(2)
    start(24)
    give(0, (0, 1))
    lay(24)
    turned(1)

    @pl.when(down)
    def _():
        edge(-1).wait_recv()

    lay(40)
    turned(3)

    def tile(j):
        return pl.ds(pl.multiple_of(j * 8, 8), 8)

    def own_rows(j):
        for i, s in enumerate(windows([tf[i, tile(j), :] for i in range(32)], 24)):
            rowmean[i, tile(j), :] = s

    def guided_rows(j):
        for i, s in enumerate(windows([tf[i, tile(j), :] * gb[i, tile(j), :] for i in range(32)], 24)):
            rowbox[i, tile(j), :] = s

    pl.loop(1, 17, unroll=2)(own_rows)

    def final(late, of, to):
        rows = pl.ds(pl.multiple_of(8 - first if late else first, 8), 8)
        return pltpu.make_async_remote_copy(
            src_ref=fin.at[:, rows, :],
            dst_ref=out.at[:, rows, pl.ds(pl.multiple_of(snake(of) * LANES, LANES), LANES)],
            send_sem=fin_send.at[late, to],
            recv_sem=fin_recv.at[late, of],
            device_id={"frame": to, "row": r},
            device_id_type=MESH,
        )

    for e in range(ROUNDS):
        take(e)
        near = jnp.concatenate([est[e, 0], est[e, 1], est[e, 2]], axis=1)
        guide = pltpu.roll(near, 3 * LANES - 120, 1)[:, 0 : 2 * LANES]

        def smooth(x):
            x = across_sum(x)
            two = x[0:47] + x[1:48]
            four = two[0:45] + two[2:47]
            return (four[0:40] + four[4:44] + x[8:48]) / cells

        mean_guide = smooth(guide)
        variance = smooth(guide * guide) - mean_guide * mean_guide
        guide_t[...] = stacked(guide)
        stat_t[...] = stacked(mean_guide, inside / (variance + GUIDE_EPS))

        @pl.loop(0, 16, unroll=16)
        def _(q):
            two = jnp.dot(guide_t[...], pick_g[q], preferred_element_type=jnp.float32)
            gb[2 * q] = two[:, 0:LANES]
            gb[2 * q + 1] = two[:, LANES:]

        pl.loop(1, 17, unroll=4)(guided_rows)

        if e == 0:
            for dc in (-1, 1):

                @pl.when(there(0, -dc))
                def _(dc=dc):
                    for q in range(4):
                        side(q, dc).wait_recv()

            own_rows(0)
            own_rows(17)

            @pl.loop(0, 24, unroll=4)
            def _(i):
                mean[i] = down_sum(rowmean[i]) * area[i]

        guided_rows(0)
        guided_rows(17)

        @pl.loop(0, 24, unroll=12)
        def _(i):
            both = jnp.dot(stat_t[...], pick_s[i], preferred_element_type=jnp.float32)
            guided = both[0:136, 0:LANES]
            m = mean[i]
            sl = (down_sum(rowbox[i]) * area[i] - guided * m) * both[0:136, LANES:]
            slope[i] = sl
            offset[i] = m - sl * guided

        @pl.loop(0, 17, unroll=17)
        def _(j):
            at = pl.ds(pl.multiple_of(j * 8, 8), 8)
            for src, dst in ((slope, box1), (offset, box2)):
                for i, s in enumerate(windows([src[i, at, :] for i in range(24)], 16)):
                    dst[i, at, :] = s

        wide = lax.broadcasted_iota(jnp.int32, (LANES, LANES), 1)
        upper = wide % HALF >= 32

        def weigh(i, acc):
            center = gb[8 + i, 8:136, :]
            filtered = (down_sum(box1[i]) * center + down_sum(box2[i])) * area[i + 4, 4:132, :]
            gap = (filtered - center) * (1.0 / CAUCHY_SCALE)
            w = 1.0 / (1.0 + gap * gap)
            wp = w * tf[i + 8, 8:136, :]
            part_sums = jnp.where(upper, w + pltpu.roll(w, 32, 1), wp + pltpu.roll(wp, 96, 1))
            return acc + jnp.dot(
                jnp.concatenate(thirds(part_sums), axis=1),
                pick_w[i],
                preferred_element_type=jnp.float32,
            )

        for late, at in enumerate((first, 8 - first)):
            at = pl.multiple_of(at, 8)
            turned_sums[...] = lax.fori_loop(
                0,
                8,
                lambda i, acc: weigh(at + i, acc),
                jnp.zeros((LANES, LANES), jnp.float32),
                unroll=8,
            ).T
            for half in range(2):
                total = turned_sums[pl.ds(half * HALF + at, 8), :]
                new = turned_sums[pl.ds(half * HALF + 16 + at, 8), :] / total
                if e < ROUNDS - 1:
                    est[e + 1, 1, pl.ds(8 + half * PAIR + at, 8), :] = new
                else:
                    fin[half, pl.ds(at, 8), :] = new
            if e < ROUNDS - 1:
                give_rows(e + 1, bool(late))
                if late:
                    give(e + 1, (0, 1))
            else:

                @pl.loop(1, nf)
                def _(s, late=late):
                    final(late, f, (f + step_of(s)) % nf).start()

    mine = pltpu.make_async_copy(
        fin, out.at[:, :, pl.ds(pl.multiple_of(c * LANES, LANES), LANES)], own_sem
    )
    mine.start()

    for k in order:

        @pl.loop(1, nf)
        def _(s, k=k):
            block(k, f, (f + s) % nf).wait_send()

    for dr in (-1, 1):

        @pl.when(there(dr, 0))
        def _(dr=dr):
            edge(dr).wait_send()

    for dc in (-1, 1):

        @pl.when(there(0, dc))
        def _(dc=dc):
            for q in range(4):
                side(q, dc).wait_send()

    for e in range(ROUNDS):
        for way, (dr, dc) in enumerate(WAYS):

            @pl.when(there(dr, dc))
            def _(e=e, way=way):
                part(e, way).wait_send()

    @pl.loop(1, nf)
    def _(s):
        peer = (f + s) % nf
        for late in range(2):
            final(late, peer, peer).wait_recv()
            final(late, f, peer).wait_send()

    mine.wait()


def merge(nf, nr, frames):
    f32 = jnp.float32
    dma = pltpu.SemaphoreType.DMA
    return pl.pallas_call(
        functools.partial(kernel, nf, nr),
        out_shape=jax.ShapeDtypeStruct((2, PAIR, nf * LANES), f32),
        in_specs=[pl.BlockSpec(memory_space=pl.ANY)],
        out_specs=pl.BlockSpec(memory_space=pl.ANY),
        scratch_shapes=[
            pltpu.VMEM((FRAMES, WIN, LANES), f32),
            pltpu.VMEM((FRAMES * PITCH, LANES), f32),
            pltpu.VMEM((32, 144, LANES), f32),
            pltpu.VMEM((24, 144, LANES), f32),
            pltpu.VMEM((24, 144, LANES), f32),
            pltpu.VMEM((24, 136, LANES), f32),
            pltpu.VMEM((24, 136, LANES), f32),
            pltpu.VMEM((24, 136, LANES), f32),
            pltpu.VMEM((24, 136, LANES), f32),
            pltpu.VMEM((16, 136, LANES), f32),
            pltpu.VMEM((16, 136, LANES), f32),
            pltpu.VMEM((144, LANES), f32),
            pltpu.VMEM((32, 144, LANES), f32),
            pltpu.VMEM((144, 256), jnp.bfloat16),
            pltpu.VMEM((144, 256), jnp.bfloat16),
            pltpu.VMEM((16, 256, 256), jnp.bfloat16),
            pltpu.VMEM((24, 256, 256), jnp.bfloat16),
            pltpu.VMEM((16, 384, LANES), jnp.bfloat16),
            pltpu.VMEM((ROUNDS, 3, WIN, LANES), f32),
            pltpu.VMEM((2, PAIR, LANES), f32),
            pltpu.VMEM((LANES, LANES), f32),
            dma,
            dma((4, nf)),
            dma((4, nf)),
            dma((2,)),
            dma((2,)),
            dma((2, 4)),
            dma((2, 4)),
            dma((ROUNDS, 8)),
            dma((ROUNDS, 8)),
            dma((2, nf)),
            dma((2, nf)),
        ],
        compiler_params=pltpu.CompilerParams(collective_id=0, has_side_effects=True),
        name="merge",
    )(frames).reshape(ROWS, nf * LANES)


def solution(mesh):
    return jax.shard_map(
        functools.partial(merge, mesh.shape["frame"], mesh.shape["row"]),
        mesh=mesh,
        in_specs=(P("frame", "row", None),),
        out_specs=P("row", None),
        check_vma=False,
    )
```

```python
import functools

import jax
import jax.numpy as jnp
from jax import lax
from jax.experimental import pallas as pl
from jax.experimental.pallas import tpu as pltpu
from jax.sharding import PartitionSpec as P

FRAMES = 64
ROUNDS = 3
GUIDE_EPS = 0.05
CAUCHY_SCALE = 0.5

LANES = 128
ROWS = 32
WIN = ROWS + 16
PITCH = 56
HALF = 64
PAIR = 16
CHUNK = 8
MESH = pl.DeviceIdType.MESH

WAYS = ((0, -1), (0, 1), (-1, 0), (1, 0), (-1, -1), (-1, 1), (1, -1), (1, 1))


def snake(i):
    z = i // 2
    return z * 2 + (i % 2 + z) % 2


def windows(a, count):
    two = [a[i] + a[i + 1] for i in range(count + 6)]
    four = [two[i] + two[i + 2] for i in range(count + 4)]
    return [(four[i] + four[i + 4]) + a[i + 8] for i in range(count)]


def down_sum(x):
    n = x.shape[0]
    two = x + pltpu.roll(x, n - 1, 0)
    four = two + pltpu.roll(two, n - 2, 0)
    eight = four + pltpu.roll(four, n - 4, 0)
    return eight[: n - 8] + x[8:]


def across_sum(x):
    n = x.shape[1]
    two = x + pltpu.roll(x, n - 1, 1)
    four = two + pltpu.roll(two, n - 2, 1)
    eight = four + pltpu.roll(four, n - 4, 1)
    return eight + pltpu.roll(x, n - 8, 1)


def thirds(x):
    high = x.astype(jnp.bfloat16)
    rest = x - high.astype(jnp.float32)
    mid = rest.astype(jnp.bfloat16)
    return high, mid, (rest - mid.astype(jnp.float32)).astype(jnp.bfloat16)


def stacked(*arrays):
    rows = [t.astype(jnp.float32) for a in arrays for t in thirds(a)]
    spare = 256 - sum(t.shape[0] for t in rows)
    rows.append(jnp.zeros((spare, rows[0].shape[1]), jnp.float32))
    return jnp.concatenate(rows, axis=0).astype(jnp.bfloat16).T[0:144]


def window_count(place, limit):
    lower = jnp.maximum(place - 4, 0)
    upper = jnp.minimum(place + 4, limit - 1)
    return jnp.maximum(upper - lower + 1, 1).astype(jnp.float32)


def kernel(
    nf, nr, frames, out, recv, flat, tf, rowbox, rowmean, mean, area, slope, offset, box1, box2,
    table, gb, guide_t, stat_t, pick_g, pick_s, pick_w, est, fin, turned_sums, own_sem, a2a_send, a2a_recv, row_send, row_recv, col_send,
    col_recv, est_send, est_recv, fin_send, fin_recv,
):
    per = FRAMES // nf
    f = lax.axis_index("frame")
    r = lax.axis_index("row")
    c = snake(f)
    up, down = r > 0, r < nr - 1
    left, right = c > 0, c < nf - 1
    odd = r % 2 == 1
    first = 8 * (r % 2)
    left_f = snake(jnp.maximum(c - 1, 0))
    right_f = snake(jnp.minimum(c + 1, nf - 1))

    def there(dr, dc):
        ok = None
        for test, step in ((up, dr == -1), (down, dr == 1), (left, dc == -1), (right, dc == 1)):
            if step:
                ok = test if ok is None else jnp.logical_and(ok, test)
        return ok

    def device(dr, dc):
        return {
            "frame": f if dc == 0 else (left_f if dc < 0 else right_f),
            "row": jnp.clip(r + dr, 0, nr - 1),
        }

    own = pltpu.make_async_copy(
        frames.at[:, :, pl.ds(pl.multiple_of(c * LANES, LANES), LANES)],
        recv.at[pl.ds(f * per, per), pl.ds(8, ROWS), :],
        own_sem,
    )
    own.start()

    @pl.when(jnp.logical_not(up))
    def _():
        recv[:, 0:8, :] = jnp.zeros((FRAMES, 8, LANES), jnp.float32)
        est[:, :, 0:8, :] = jnp.zeros((ROUNDS, 3, 8, LANES), jnp.float32)

    @pl.when(jnp.logical_not(down))
    def _():
        recv[:, 40:48, :] = jnp.zeros((FRAMES, 8, LANES), jnp.float32)
        est[:, :, 40:48, :] = jnp.zeros((ROUNDS, 3, 8, LANES), jnp.float32)

    @pl.when(jnp.logical_not(left))
    def _():
        tf[:, 0:8, :] = jnp.zeros((32, 8, LANES), jnp.float32)
        est[:, 0] = jnp.zeros((ROUNDS, WIN, LANES), jnp.float32)

    @pl.when(jnp.logical_not(right))
    def _():
        tf[:, 136:144, :] = jnp.zeros((32, 8, LANES), jnp.float32)
        est[:, 2] = jnp.zeros((ROUNDS, WIN, LANES), jnp.float32)

    def step_of(s):
        d = (s + 1) // 2
        return jnp.where(s % 2 == 1, d, nf - d)

    barrier = pltpu.get_barrier_semaphore()

    @pl.loop(1, nf)
    def _(s):
        pl.semaphore_signal(
            barrier, inc=1, device_id={"frame": (f + step_of(nf - s)) % nf, "row": r}, device_id_type=MESH
        )

    others = jnp.int32(nf - 1)
    for dr, dc in WAYS:
        if dr == 0:
            continue

        @pl.when(there(dr, dc))
        def _(dr=dr, dc=dc):
            pl.semaphore_signal(barrier, inc=1, device_id=device(dr, dc), device_id_type=MESH)

        others = others + there(dr, dc).astype(jnp.int32)
    pl.semaphore_wait(barrier, others)

    def block(k, peer, to):
        return pltpu.make_async_remote_copy(
            src_ref=frames.at[
                :, pl.ds(k * CHUNK, CHUNK), pl.ds(pl.multiple_of(snake(to) * LANES, LANES), LANES)
            ],
            dst_ref=recv.at[pl.ds(peer * per, per), pl.ds(8 + k * CHUNK, CHUNK), :],
            send_sem=a2a_send.at[k, to],
            recv_sem=a2a_recv.at[k, peer],
            device_id={"frame": to, "row": r},
            device_id_type=MESH,
        )

    order = (0, 3, 1, 2)
    for k in order:

        @pl.loop(1, nf)
        def _(s, k=k):
            block(k, f, (f + step_of(nf - s)) % nf).start()

    def arrived(k):
        @pl.loop(1, nf)
        def _(s):
            peer = (f + s) % nf
            block(k, peer, peer).wait_recv()

    def edge(dr):
        at, to = (8, 40) if dr < 0 else (32, 0)
        i = 0 if dr < 0 else 1
        return pltpu.make_async_remote_copy(
            src_ref=recv.at[:, pl.ds(at, 8), :],
            dst_ref=recv.at[:, pl.ds(to, 8), :],
            send_sem=row_send.at[i],
            recv_sem=row_recv.at[i],
            device_id=device(dr, 0),
            device_id_type=MESH,
        )

    lane = lax.broadcasted_iota(jnp.int32, (8, LANES), 1)
    second = jnp.where(lane >= HALF, PAIR, 0)
    height, width = nr * ROWS, nf * LANES
    place_r = r * ROWS - 4 + lax.broadcasted_iota(jnp.int32, (40, 2 * LANES), 0)
    place_c = c * LANES - 4 + lax.broadcasted_iota(jnp.int32, (40, 2 * LANES), 1)
    cells = window_count(place_r, height) * window_count(place_c, width)
    inside = jnp.where(
        (place_r >= 0) & (place_r < height) & (place_c >= 0) & (place_c < width), 1.0, 0.0
    )
    share = 1.0 / cells

    def keep(top, mid, low):
        both = jnp.concatenate([top, mid, low], axis=0)
        table[0:LANES, :] = both[:, 0:LANES].T
        table[LANES : LANES + 16, :] = both[:, LANES : 2 * LANES].T[0:16]

    def spread(x, row):
        idx = jnp.broadcast_to((second + row)[0:1], x.shape)
        return jnp.take_along_axis(x, idx, axis=1, mode="promise_in_bounds")

    zeros48 = jnp.zeros((WIN, 2 * LANES), jnp.float32)
    keep(zeros48, share * inside, share)

    @pl.loop(0, 24)
    def _(i):
        area[i] = spread(table[0:136, :], 48 + i)

    k = lax.broadcasted_iota(jnp.int32, (256, 256), 0)
    n = lax.broadcasted_iota(jnp.int32, (256, 256), 1)
    side_n, half_n = n // LANES, jnp.where(n % LANES >= HALF, PAIR, 0)
    row_g = jnp.where(k < 144, k % 48, 255) - half_n - side_n
    row_s = jnp.where(k // 120 == side_n, k % 40, 255) - half_n

    @pl.loop(0, 16)
    def _(q):
        pick_g[q] = jnp.where(row_g == 2 * q, 1.0, 0.0).astype(jnp.bfloat16)

    @pl.loop(0, 24)
    def _(i):
        pick_s[i] = jnp.where(row_s == i, 1.0, 0.0).astype(jnp.bfloat16)

    k = lax.broadcasted_iota(jnp.int32, (384, LANES), 0) % LANES
    n = lax.broadcasted_iota(jnp.int32, (384, LANES), 1)
    row_w = n - jnp.where(k >= HALF, HALF, 0) - jnp.where(k % HALF >= 32, 0, 16)

    @pl.loop(0, PAIR)
    def _(i):
        pick_w[i] = jnp.where(row_w == i, 1.0, 0.0).astype(jnp.bfloat16)

    own.wait()
    arrived(0)

    @pl.when(up)
    def _():
        edge(-1).start()

    arrived(3)

    @pl.when(down)
    def _():
        edge(1).start()

    def lay(at):
        @pl.loop(0, FRAMES, unroll=8)
        def _(p):
            flat[pl.ds(pl.multiple_of(p * PITCH + at, 8), 8), :] = recv[p, at : at + 8, :]

    def turn(q):
        @pl.loop(0, 8, unroll=8)
        def _(i):
            row = q * 8 + i
            a = flat[pl.ds(row, FRAMES, stride=PITCH), :]
            b = flat[pl.ds(row + PAIR, FRAMES, stride=PITCH), :]
            tf[row, 8:136, :] = jnp.concatenate([a, b], axis=0).T

    def side(q, dc):
        at, to = (8, 136) if dc < 0 else (128, 0)
        i = 0 if dc < 0 else 1
        return pltpu.make_async_remote_copy(
            src_ref=tf.at[pl.ds(q * 8, 8), pl.ds(at, 8), :],
            dst_ref=tf.at[pl.ds(q * 8, 8), pl.ds(to, 8), :],
            send_sem=col_send.at[i, q],
            recv_sem=col_recv.at[i, q],
            device_id=device(0, dc),
            device_id_type=MESH,
        )

    def turned(q):
        turn(q)
        for dc in (-1, 1):

            @pl.when(there(0, dc))
            def _(dc=dc):
                side(q, dc).start()

    lay(8)
    lay(32)
    def part(e, way):
        dr, dc = WAYS[way]
        at, size, to = {0: (8, ROWS, 8), -1: (8, 8, 40), 1: (32, 8, 0)}[dr]
        return pltpu.make_async_remote_copy(
            src_ref=est.at[e, 1, pl.ds(at, size), :],
            dst_ref=est.at[e, 1 - dc, pl.ds(to, size), :],
            send_sem=est_send.at[e, way],
            recv_sem=est_recv.at[e, way],
            device_id=device(dr, dc),
            device_id_type=MESH,
        )

    def give(e, ways):
        for way in ways:

            @pl.when(there(*WAYS[way]))
            def _(way=way):
                part(e, way).start()

    def give_rows(e, late):
        @pl.when(odd != late)
        def _():
            give(e, (3, 6, 7))

        @pl.when(odd == late)
        def _():
            give(e, (2, 4, 5))

    def take(e):
        for way, (dr, dc) in enumerate(WAYS):

            @pl.when(there(-dr, -dc))
            def _(way=way):
                part(e, way).wait_recv()

    def start(at):
        total = lax.fori_loop(
            0, FRAMES, lambda p, t: t + recv[p, at : at + 8, :], jnp.zeros((8, LANES), jnp.float32),
            unroll=16,
        )
        est[0, 1, at : at + 8, :] = total / FRAMES

    start(8)
    start(32)
    give_rows(0, False)
    give_rows(0, True)
    arrived(1)
    start(16)
    lay(16)
    turned(2)

    @pl.when(up)
    def _():
        edge(1).wait_recv()

    lay(0)
    turned(0)
    @pl.when(down)
    def _():
        edge(-1).wait_recv()

    lay(40)
    arrived(2)
    start(24)
    give(0, (0, 1))
    lay(24)
    turned(1)

    turned(3)

    def tile(j):
        return pl.ds(pl.multiple_of(j * 8, 8), 8)

    def own_rows(j):
        for i, s in enumerate(windows([tf[i, tile(j), :] for i in range(32)], 24)):
            rowmean[i, tile(j), :] = s

    def guided_rows(j):
        for i, s in enumerate(windows([tf[i, tile(j), :] * gb[i, tile(j), :] for i in range(32)], 24)):
            rowbox[i, tile(j), :] = s

    pl.loop(1, 17, unroll=2)(own_rows)

    def final(late, of, to):
        rows = pl.ds(pl.multiple_of(8 - first if late else first, 8), 8)
        return pltpu.make_async_remote_copy(
            src_ref=fin.at[:, rows, :],
            dst_ref=out.at[:, rows, pl.ds(pl.multiple_of(snake(of) * LANES, LANES), LANES)],
            send_sem=fin_send.at[late, to],
            recv_sem=fin_recv.at[late, of],
            device_id={"frame": to, "row": r},
            device_id_type=MESH,
        )

    for e in range(ROUNDS):
        take(e)
        near = jnp.concatenate([est[e, 0], est[e, 1], est[e, 2]], axis=1)
        guide = pltpu.roll(near, 3 * LANES - 120, 1)[:, 0 : 2 * LANES]

        def smooth(x):
            x = across_sum(x)
            two = x[0:47] + x[1:48]
            four = two[0:45] + two[2:47]
            return (four[0:40] + four[4:44] + x[8:48]) / cells

        mean_guide = smooth(guide)
        variance = smooth(guide * guide) - mean_guide * mean_guide
        guide_t[...] = stacked(guide)
        stat_t[...] = stacked(mean_guide, inside / (variance + GUIDE_EPS))

        @pl.loop(0, 16, unroll=16)
        def _(q):
            two = jnp.dot(guide_t[...], pick_g[q], preferred_element_type=jnp.float32)
            gb[2 * q] = two[:, 0:LANES]
            gb[2 * q + 1] = two[:, LANES:]

        pl.loop(1, 17, unroll=4)(guided_rows)

        if e == 0:
            for dc in (-1, 1):

                @pl.when(there(0, -dc))
                def _(dc=dc):
                    for q in range(4):
                        side(q, dc).wait_recv()

            own_rows(0)
            own_rows(17)

            @pl.loop(0, 24, unroll=4)
            def _(i):
                mean[i] = down_sum(rowmean[i]) * area[i]

        guided_rows(0)
        guided_rows(17)

        @pl.loop(0, 24, unroll=24)
        def _(i):
            both = jnp.dot(stat_t[...], pick_s[i], preferred_element_type=jnp.float32)
            guided = both[0:136, 0:LANES]
            m = mean[i]
            sl = (down_sum(rowbox[i]) * area[i] - guided * m) * both[0:136, LANES:]
            slope[i] = sl
            offset[i] = m - sl * guided

        @pl.loop(0, 17, unroll=17)
        def _(j):
            at = pl.ds(pl.multiple_of(j * 8, 8), 8)
            for src, dst in ((slope, box1), (offset, box2)):
                for i, s in enumerate(windows([src[i, at, :] for i in range(24)], 16)):
                    dst[i, at, :] = s

        wide = lax.broadcasted_iota(jnp.int32, (LANES, LANES), 1)
        upper = wide % HALF >= 32

        def weigh(i, acc):
            center = gb[8 + i, 8:136, :]
            filtered = (down_sum(box1[i]) * center + down_sum(box2[i])) * area[i + 4, 4:132, :]
            gap = (filtered - center) * (1.0 / CAUCHY_SCALE)
            w = 1.0 / (1.0 + gap * gap)
            wp = w * tf[i + 8, 8:136, :]
            part_sums = jnp.where(upper, w + pltpu.roll(w, 32, 1), wp + pltpu.roll(wp, 96, 1))
            return acc + jnp.dot(
                jnp.concatenate(thirds(part_sums), axis=1),
                pick_w[i],
                preferred_element_type=jnp.float32,
            )

        for late, at in enumerate((first, 8 - first)):
            at = pl.multiple_of(at, 8)
            turned_sums[...] = lax.fori_loop(
                0,
                8,
                lambda i, acc: weigh(at + i, acc),
                jnp.zeros((LANES, LANES), jnp.float32),
                unroll=8,
            ).T
            for half in range(2):
                total = turned_sums[pl.ds(half * HALF + at, 8), :]
                new = turned_sums[pl.ds(half * HALF + 16 + at, 8), :] / total
                if e < ROUNDS - 1:
                    est[e + 1, 1, pl.ds(8 + half * PAIR + at, 8), :] = new
                else:
                    fin[half, pl.ds(at, 8), :] = new
            if e < ROUNDS - 1:
                give_rows(e + 1, bool(late))
                if late:
                    give(e + 1, (0, 1))
            else:

                @pl.loop(1, nf)
                def _(s, late=late):
                    final(late, f, (f + step_of(nf - s)) % nf).start()

    mine = pltpu.make_async_copy(
        fin, out.at[:, :, pl.ds(pl.multiple_of(c * LANES, LANES), LANES)], own_sem
    )
    mine.start()

    for k in order:

        @pl.loop(1, nf)
        def _(s, k=k):
            block(k, f, (f + s) % nf).wait_send()

    for dr in (-1, 1):

        @pl.when(there(dr, 0))
        def _(dr=dr):
            edge(dr).wait_send()

    for dc in (-1, 1):

        @pl.when(there(0, dc))
        def _(dc=dc):
            for q in range(4):
                side(q, dc).wait_send()

    for e in range(ROUNDS):
        for way, (dr, dc) in enumerate(WAYS):

            @pl.when(there(dr, dc))
            def _(e=e, way=way):
                part(e, way).wait_send()

    @pl.loop(1, nf)
    def _(s):
        peer = (f + s) % nf
        for late in range(2):
            final(late, peer, peer).wait_recv()
            final(late, f, peer).wait_send()

    mine.wait()


def merge(nf, nr, frames):
    f32 = jnp.float32
    dma = pltpu.SemaphoreType.DMA
    return pl.pallas_call(
        functools.partial(kernel, nf, nr),
        out_shape=jax.ShapeDtypeStruct((2, PAIR, nf * LANES), f32),
        in_specs=[pl.BlockSpec(memory_space=pl.ANY)],
        out_specs=pl.BlockSpec(memory_space=pl.ANY),
        scratch_shapes=[
            pltpu.VMEM((FRAMES, WIN, LANES), f32),
            pltpu.VMEM((FRAMES * PITCH, LANES), f32),
            pltpu.VMEM((32, 144, LANES), f32),
            pltpu.VMEM((24, 144, LANES), f32),
            pltpu.VMEM((24, 144, LANES), f32),
            pltpu.VMEM((24, 136, LANES), f32),
            pltpu.VMEM((24, 136, LANES), f32),
            pltpu.VMEM((24, 136, LANES), f32),
            pltpu.VMEM((24, 136, LANES), f32),
            pltpu.VMEM((16, 136, LANES), f32),
            pltpu.VMEM((16, 136, LANES), f32),
            pltpu.VMEM((144, LANES), f32),
            pltpu.VMEM((32, 144, LANES), f32),
            pltpu.VMEM((144, 256), jnp.bfloat16),
            pltpu.VMEM((144, 256), jnp.bfloat16),
            pltpu.VMEM((16, 256, 256), jnp.bfloat16),
            pltpu.VMEM((24, 256, 256), jnp.bfloat16),
            pltpu.VMEM((16, 384, LANES), jnp.bfloat16),
            pltpu.VMEM((ROUNDS, 3, WIN, LANES), f32),
            pltpu.VMEM((2, PAIR, LANES), f32),
            pltpu.VMEM((LANES, LANES), f32),
            dma,
            dma((4, nf)),
            dma((4, nf)),
            dma((2,)),
            dma((2,)),
            dma((2, 4)),
            dma((2, 4)),
            dma((ROUNDS, 8)),
            dma((ROUNDS, 8)),
            dma((2, nf)),
            dma((2, nf)),
        ],
        compiler_params=pltpu.CompilerParams(collective_id=0, has_side_effects=True),
        name="merge",
    )(frames).reshape(ROWS, nf * LANES)


def solution(mesh):
    return jax.shard_map(
        functools.partial(merge, mesh.shape["frame"], mesh.shape["row"]),
        mesh=mesh,
        in_specs=(P("frame", "row", None),),
        out_specs=P("row", None),
        check_vma=False,
    )
```

```python
import functools

import jax
import jax.numpy as jnp
from jax import lax
from jax.experimental import pallas as pl
from jax.experimental.pallas import tpu as pltpu
from jax.sharding import PartitionSpec as P

FRAMES = 64
ROUNDS = 3
GUIDE_EPS = 0.05
CAUCHY_SCALE = 0.5

LANES = 128
ROWS = 32
WIN = ROWS + 16
PITCH = 56
HALF = 64
PAIR = 16
CHUNK = 8
MESH = pl.DeviceIdType.MESH

WAYS = ((0, -1), (0, 1), (-1, 0), (1, 0), (-1, -1), (-1, 1), (1, -1), (1, 1))


def snake(i):
    z = i // 2
    return z * 2 + (i % 2 + z) % 2


def windows(a, count):
    two = [a[i] + a[i + 1] for i in range(count + 6)]
    four = [two[i] + two[i + 2] for i in range(count + 4)]
    return [(four[i] + four[i + 4]) + a[i + 8] for i in range(count)]


def down_sum(x):
    n = x.shape[0]
    two = x + pltpu.roll(x, n - 1, 0)
    four = two + pltpu.roll(two, n - 2, 0)
    eight = four + pltpu.roll(four, n - 4, 0)
    return eight[: n - 8] + x[8:]


def across_sum(x):
    n = x.shape[1]
    two = x + pltpu.roll(x, n - 1, 1)
    four = two + pltpu.roll(two, n - 2, 1)
    eight = four + pltpu.roll(four, n - 4, 1)
    return eight + pltpu.roll(x, n - 8, 1)


def thirds(x):
    high = x.astype(jnp.bfloat16)
    rest = x - high.astype(jnp.float32)
    mid = rest.astype(jnp.bfloat16)
    return high, mid, (rest - mid.astype(jnp.float32)).astype(jnp.bfloat16)


def stacked(*arrays):
    rows = [t.astype(jnp.float32) for a in arrays for t in thirds(a)]
    spare = 256 - sum(t.shape[0] for t in rows)
    rows.append(jnp.zeros((spare, rows[0].shape[1]), jnp.float32))
    return jnp.concatenate(rows, axis=0).astype(jnp.bfloat16).T[0:144]


def window_count(place, limit):
    lower = jnp.maximum(place - 4, 0)
    upper = jnp.minimum(place + 4, limit - 1)
    return jnp.maximum(upper - lower + 1, 1).astype(jnp.float32)


def kernel(
    nf, nr, frames, out, recv, flat, tf, rowbox, rowmean, mean, area, slope, offset, box1, box2,
    table, gb, guide_t, stat_t, pick_g, pick_s, pick_w, est, fin, turned_sums, own_sem, a2a_send, a2a_recv, row_send, row_recv, col_send,
    col_recv, est_send, est_recv, fin_send, fin_recv,
):
    per = FRAMES // nf
    f = lax.axis_index("frame")
    r = lax.axis_index("row")
    c = snake(f)
    up, down = r > 0, r < nr - 1
    left, right = c > 0, c < nf - 1
    odd = r % 2 == 1
    first = 8 * (r % 2)
    left_f = snake(jnp.maximum(c - 1, 0))
    right_f = snake(jnp.minimum(c + 1, nf - 1))

    def there(dr, dc):
        ok = None
        for test, step in ((up, dr == -1), (down, dr == 1), (left, dc == -1), (right, dc == 1)):
            if step:
                ok = test if ok is None else jnp.logical_and(ok, test)
        return ok

    def device(dr, dc):
        return {
            "frame": f if dc == 0 else (left_f if dc < 0 else right_f),
            "row": jnp.clip(r + dr, 0, nr - 1),
        }

    own = pltpu.make_async_copy(
        frames.at[:, :, pl.ds(pl.multiple_of(c * LANES, LANES), LANES)],
        recv.at[pl.ds(f * per, per), pl.ds(8, ROWS), :],
        own_sem,
    )
    own.start()

    @pl.when(jnp.logical_not(up))
    def _():
        recv[:, 0:8, :] = jnp.zeros((FRAMES, 8, LANES), jnp.float32)
        est[:, :, 0:8, :] = jnp.zeros((ROUNDS, 3, 8, LANES), jnp.float32)

    @pl.when(jnp.logical_not(down))
    def _():
        recv[:, 40:48, :] = jnp.zeros((FRAMES, 8, LANES), jnp.float32)
        est[:, :, 40:48, :] = jnp.zeros((ROUNDS, 3, 8, LANES), jnp.float32)

    @pl.when(jnp.logical_not(left))
    def _():
        tf[:, 0:8, :] = jnp.zeros((32, 8, LANES), jnp.float32)
        est[:, 0] = jnp.zeros((ROUNDS, WIN, LANES), jnp.float32)

    @pl.when(jnp.logical_not(right))
    def _():
        tf[:, 136:144, :] = jnp.zeros((32, 8, LANES), jnp.float32)
        est[:, 2] = jnp.zeros((ROUNDS, WIN, LANES), jnp.float32)

    def step_of(s):
        d = (s + 1) // 2
        return jnp.where(s % 2 == 1, d, nf - d)

    barrier = pltpu.get_barrier_semaphore()

    @pl.loop(1, nf)
    def _(s):
        pl.semaphore_signal(
            barrier, inc=1, device_id={"frame": (f + step_of(nf - s)) % nf, "row": r}, device_id_type=MESH
        )

    others = jnp.int32(nf - 1)
    for dr, dc in WAYS:
        if dr == 0:
            continue

        @pl.when(there(dr, dc))
        def _(dr=dr, dc=dc):
            pl.semaphore_signal(barrier, inc=1, device_id=device(dr, dc), device_id_type=MESH)

        others = others + there(dr, dc).astype(jnp.int32)
    pl.semaphore_wait(barrier, others)

    def block(k, peer, to):
        return pltpu.make_async_remote_copy(
            src_ref=frames.at[
                :, pl.ds(k * CHUNK, CHUNK), pl.ds(pl.multiple_of(snake(to) * LANES, LANES), LANES)
            ],
            dst_ref=recv.at[pl.ds(peer * per, per), pl.ds(8 + k * CHUNK, CHUNK), :],
            send_sem=a2a_send.at[k, to],
            recv_sem=a2a_recv.at[k, peer],
            device_id={"frame": to, "row": r},
            device_id_type=MESH,
        )

    order = (0, 3, 1, 2)
    for k in order:

        @pl.loop(1, nf)
        def _(s, k=k):
            block(k, f, (f + step_of(nf - s)) % nf).start()

    def arrived(k):
        @pl.loop(1, nf)
        def _(s):
            peer = (f + s) % nf
            block(k, peer, peer).wait_recv()

    def edge(dr):
        at, to = (8, 40) if dr < 0 else (32, 0)
        i = 0 if dr < 0 else 1
        return pltpu.make_async_remote_copy(
            src_ref=recv.at[:, pl.ds(at, 8), :],
            dst_ref=recv.at[:, pl.ds(to, 8), :],
            send_sem=row_send.at[i],
            recv_sem=row_recv.at[i],
            device_id=device(dr, 0),
            device_id_type=MESH,
        )

    lane = lax.broadcasted_iota(jnp.int32, (8, LANES), 1)
    second = jnp.where(lane >= HALF, PAIR, 0)
    height, width = nr * ROWS, nf * LANES
    place_r = r * ROWS - 4 + lax.broadcasted_iota(jnp.int32, (40, 2 * LANES), 0)
    place_c = c * LANES - 4 + lax.broadcasted_iota(jnp.int32, (40, 2 * LANES), 1)
    cells = window_count(place_r, height) * window_count(place_c, width)
    inside = jnp.where(
        (place_r >= 0) & (place_r < height) & (place_c >= 0) & (place_c < width), 1.0, 0.0
    )
    share = 1.0 / cells

    def keep(top, mid, low):
        both = jnp.concatenate([top, mid, low], axis=0)
        table[0:LANES, :] = both[:, 0:LANES].T
        table[LANES : LANES + 16, :] = both[:, LANES : 2 * LANES].T[0:16]

    def spread(x, row):
        idx = jnp.broadcast_to((second + row)[0:1], x.shape)
        return jnp.take_along_axis(x, idx, axis=1, mode="promise_in_bounds")

    zeros48 = jnp.zeros((WIN, 2 * LANES), jnp.float32)
    keep(zeros48, share * inside, share)

    @pl.loop(0, 24)
    def _(i):
        area[i] = spread(table[0:136, :], 48 + i)

    k = lax.broadcasted_iota(jnp.int32, (256, 256), 0)
    n = lax.broadcasted_iota(jnp.int32, (256, 256), 1)
    side_n, half_n = n // LANES, jnp.where(n % LANES >= HALF, PAIR, 0)
    row_g = jnp.where(k < 144, k % 48, 255) - half_n - side_n
    row_s = jnp.where(k // 120 == side_n, k % 40, 255) - half_n

    @pl.loop(0, 16)
    def _(q):
        pick_g[q] = jnp.where(row_g == 2 * q, 1.0, 0.0).astype(jnp.bfloat16)

    @pl.loop(0, 24)
    def _(i):
        pick_s[i] = jnp.where(row_s == i, 1.0, 0.0).astype(jnp.bfloat16)

    k = lax.broadcasted_iota(jnp.int32, (384, LANES), 0) % LANES
    n = lax.broadcasted_iota(jnp.int32, (384, LANES), 1)
    row_w = n - jnp.where(k >= HALF, HALF, 0) - jnp.where(k % HALF >= 32, 0, 16)

    @pl.loop(0, PAIR)
    def _(i):
        pick_w[i] = jnp.where(row_w == i, 1.0, 0.0).astype(jnp.bfloat16)

    own.wait()
    arrived(0)

    @pl.when(up)
    def _():
        edge(-1).start()

    arrived(3)

    @pl.when(down)
    def _():
        edge(1).start()

    def lay(at):
        @pl.loop(0, FRAMES, unroll=8)
        def _(p):
            flat[pl.ds(pl.multiple_of(p * PITCH + at, 8), 8), :] = recv[p, at : at + 8, :]

    def turn(q):
        @pl.loop(0, 8, unroll=8)
        def _(i):
            row = q * 8 + i
            a = flat[pl.ds(row, FRAMES, stride=PITCH), :]
            b = flat[pl.ds(row + PAIR, FRAMES, stride=PITCH), :]
            tf[row, 8:136, :] = jnp.concatenate([a, b], axis=0).T

    def side(q, dc):
        at, to = (8, 136) if dc < 0 else (128, 0)
        i = 0 if dc < 0 else 1
        return pltpu.make_async_remote_copy(
            src_ref=tf.at[pl.ds(q * 8, 8), pl.ds(at, 8), :],
            dst_ref=tf.at[pl.ds(q * 8, 8), pl.ds(to, 8), :],
            send_sem=col_send.at[i, q],
            recv_sem=col_recv.at[i, q],
            device_id=device(0, dc),
            device_id_type=MESH,
        )

    def turned(q):
        turn(q)
        for dc in (-1, 1):

            @pl.when(there(0, dc))
            def _(dc=dc):
                side(q, dc).start()

    lay(8)
    lay(32)
    def part(e, way):
        dr, dc = WAYS[way]
        at, size, to = {0: (8, ROWS, 8), -1: (8, 8, 40), 1: (32, 8, 0)}[dr]
        return pltpu.make_async_remote_copy(
            src_ref=est.at[e, 1, pl.ds(at, size), :],
            dst_ref=est.at[e, 1 - dc, pl.ds(to, size), :],
            send_sem=est_send.at[e, way],
            recv_sem=est_recv.at[e, way],
            device_id=device(dr, dc),
            device_id_type=MESH,
        )

    def give(e, ways):
        for way in ways:

            @pl.when(there(*WAYS[way]))
            def _(way=way):
                part(e, way).start()

    def give_rows(e, late):
        @pl.when(odd != late)
        def _():
            give(e, (6, 7, 3))

        @pl.when(odd == late)
        def _():
            give(e, (4, 5, 2))

    def take(e):
        for way, (dr, dc) in enumerate(WAYS):

            @pl.when(there(-dr, -dc))
            def _(way=way):
                part(e, way).wait_recv()

    def start(at):
        total = lax.fori_loop(
            0, FRAMES, lambda p, t: t + recv[p, at : at + 8, :], jnp.zeros((8, LANES), jnp.float32),
            unroll=16,
        )
        est[0, 1, at : at + 8, :] = total / FRAMES

    start(8)
    start(32)
    give_rows(0, False)
    give_rows(0, True)
    arrived(1)
    start(16)
    lay(16)
    turned(2)

    @pl.when(up)
    def _():
        edge(1).wait_recv()

    lay(0)
    turned(0)
    @pl.when(down)
    def _():
        edge(-1).wait_recv()

    lay(40)
    arrived(2)
    start(24)
    give(0, (0, 1))
    lay(24)
    turned(1)

    turned(3)

    def tile(j):
        return pl.ds(pl.multiple_of(j * 8, 8), 8)

    def own_rows(j):
        for i, s in enumerate(windows([tf[i, tile(j), :] for i in range(32)], 24)):
            rowmean[i, tile(j), :] = s

    def guided_rows(j):
        for i, s in enumerate(windows([tf[i, tile(j), :] * gb[i, tile(j), :] for i in range(32)], 24)):
            rowbox[i, tile(j), :] = s

    pl.loop(1, 17, unroll=4)(own_rows)

    def final(late, of, to):
        rows = pl.ds(pl.multiple_of(8 - first if late else first, 8), 8)
        return pltpu.make_async_remote_copy(
            src_ref=fin.at[:, rows, :],
            dst_ref=out.at[:, rows, pl.ds(pl.multiple_of(snake(of) * LANES, LANES), LANES)],
            send_sem=fin_send.at[late, to],
            recv_sem=fin_recv.at[late, of],
            device_id={"frame": to, "row": r},
            device_id_type=MESH,
        )

    for e in range(ROUNDS):
        take(e)
        near = jnp.concatenate([est[e, 0], est[e, 1], est[e, 2]], axis=1)
        guide = pltpu.roll(near, 3 * LANES - 120, 1)[:, 0 : 2 * LANES]

        def smooth(x):
            x = across_sum(x)
            two = x[0:47] + x[1:48]
            four = two[0:45] + two[2:47]
            return (four[0:40] + four[4:44] + x[8:48]) / cells

        mean_guide = smooth(guide)
        variance = smooth(guide * guide) - mean_guide * mean_guide
        guide_t[...] = stacked(guide)
        stat_t[...] = stacked(mean_guide, inside / (variance + GUIDE_EPS))

        @pl.loop(0, 16, unroll=16)
        def _(q):
            two = jnp.dot(guide_t[...], pick_g[q], preferred_element_type=jnp.float32)
            gb[2 * q] = two[:, 0:LANES]
            gb[2 * q + 1] = two[:, LANES:]

        pl.loop(1, 17, unroll=8)(guided_rows)

        if e == 0:
            for dc in (-1, 1):

                @pl.when(there(0, -dc))
                def _(dc=dc):
                    for q in range(4):
                        side(q, dc).wait_recv()

            own_rows(0)
            own_rows(17)

            @pl.loop(0, 24, unroll=12)
            def _(i):
                mean[i] = down_sum(rowmean[i]) * area[i]

        guided_rows(0)
        guided_rows(17)

        @pl.loop(0, 24, unroll=24)
        def _(i):
            both = jnp.dot(stat_t[...], pick_s[i], preferred_element_type=jnp.float32)
            guided = both[0:136, 0:LANES]
            m = mean[i]
            sl = (down_sum(rowbox[i]) * area[i] - guided * m) * both[0:136, LANES:]
            slope[i] = sl
            offset[i] = m - sl * guided

        @pl.loop(0, 17, unroll=17)
        def _(j):
            at = pl.ds(pl.multiple_of(j * 8, 8), 8)
            for src, dst in ((slope, box1), (offset, box2)):
                for i, s in enumerate(windows([src[i, at, :] for i in range(24)], 16)):
                    dst[i, at, :] = s

        wide = lax.broadcasted_iota(jnp.int32, (LANES, LANES), 1)
        upper = wide % HALF >= 32

        def weigh(i, acc):
            center = gb[8 + i, 8:136, :]
            filtered = (down_sum(box1[i]) * center + down_sum(box2[i])) * area[i + 4, 4:132, :]
            gap = (filtered - center) * (1.0 / CAUCHY_SCALE)
            w = 1.0 / (1.0 + gap * gap)
            wp = w * tf[i + 8, 8:136, :]
            part_sums = jnp.where(upper, w + pltpu.roll(w, 32, 1), wp + pltpu.roll(wp, 96, 1))
            return acc + jnp.dot(
                jnp.concatenate(thirds(part_sums), axis=1),
                pick_w[i],
                preferred_element_type=jnp.float32,
            )

        for late, at in enumerate((first, 8 - first)):
            at = pl.multiple_of(at, 8)
            turned_sums[...] = lax.fori_loop(
                0,
                8,
                lambda i, acc: weigh(at + i, acc),
                jnp.zeros((LANES, LANES), jnp.float32),
                unroll=8,
            ).T
            for half in range(2):
                total = turned_sums[pl.ds(half * HALF + at, 8), :]
                new = turned_sums[pl.ds(half * HALF + 16 + at, 8), :] / total
                if e < ROUNDS - 1:
                    est[e + 1, 1, pl.ds(8 + half * PAIR + at, 8), :] = new
                else:
                    fin[half, pl.ds(at, 8), :] = new
            if e < ROUNDS - 1:
                give_rows(e + 1, bool(late))
                if late:
                    give(e + 1, (0, 1))
            else:

                @pl.loop(1, nf)
                def _(s, late=late):
                    final(late, f, (f + step_of(nf - s)) % nf).start()

    mine = pltpu.make_async_copy(
        fin, out.at[:, :, pl.ds(pl.multiple_of(c * LANES, LANES), LANES)], own_sem
    )
    mine.start()

    for k in order:

        @pl.loop(1, nf)
        def _(s, k=k):
            block(k, f, (f + s) % nf).wait_send()

    for dr in (-1, 1):

        @pl.when(there(dr, 0))
        def _(dr=dr):
            edge(dr).wait_send()

    for dc in (-1, 1):

        @pl.when(there(0, dc))
        def _(dc=dc):
            for q in range(4):
                side(q, dc).wait_send()

    for e in range(ROUNDS):
        for way, (dr, dc) in enumerate(WAYS):

            @pl.when(there(dr, dc))
            def _(e=e, way=way):
                part(e, way).wait_send()

    @pl.loop(1, nf)
    def _(s):
        peer = (f + s) % nf
        for late in range(2):
            final(late, peer, peer).wait_recv()
            final(late, f, peer).wait_send()

    mine.wait()


def merge(nf, nr, frames):
    f32 = jnp.float32
    dma = pltpu.SemaphoreType.DMA
    return pl.pallas_call(
        functools.partial(kernel, nf, nr),
        out_shape=jax.ShapeDtypeStruct((2, PAIR, nf * LANES), f32),
        in_specs=[pl.BlockSpec(memory_space=pl.ANY)],
        out_specs=pl.BlockSpec(memory_space=pl.ANY),
        scratch_shapes=[
            pltpu.VMEM((FRAMES, WIN, LANES), f32),
            pltpu.VMEM((FRAMES * PITCH, LANES), f32),
            pltpu.VMEM((32, 144, LANES), f32),
            pltpu.VMEM((24, 144, LANES), f32),
            pltpu.VMEM((24, 144, LANES), f32),
            pltpu.VMEM((24, 136, LANES), f32),
            pltpu.VMEM((24, 136, LANES), f32),
            pltpu.VMEM((24, 136, LANES), f32),
            pltpu.VMEM((24, 136, LANES), f32),
            pltpu.VMEM((16, 136, LANES), f32),
            pltpu.VMEM((16, 136, LANES), f32),
            pltpu.VMEM((144, LANES), f32),
            pltpu.VMEM((32, 144, LANES), f32),
            pltpu.VMEM((144, 256), jnp.bfloat16),
            pltpu.VMEM((144, 256), jnp.bfloat16),
            pltpu.VMEM((16, 256, 256), jnp.bfloat16),
            pltpu.VMEM((24, 256, 256), jnp.bfloat16),
            pltpu.VMEM((16, 384, LANES), jnp.bfloat16),
            pltpu.VMEM((ROUNDS, 3, WIN, LANES), f32),
            pltpu.VMEM((2, PAIR, LANES), f32),
            pltpu.VMEM((LANES, LANES), f32),
            dma,
            dma((4, nf)),
            dma((4, nf)),
            dma((2,)),
            dma((2,)),
            dma((2, 4)),
            dma((2, 4)),
            dma((ROUNDS, 8)),
            dma((ROUNDS, 8)),
            dma((2, nf)),
            dma((2, nf)),
        ],
        compiler_params=pltpu.CompilerParams(collective_id=0, has_side_effects=True),
        name="merge",
    )(frames).reshape(ROWS, nf * LANES)


def solution(mesh):
    return jax.shard_map(
        functools.partial(merge, mesh.shape["frame"], mesh.shape["row"]),
        mesh=mesh,
        in_specs=(P("frame", "row", None),),
        out_specs=P("row", None),
        check_vma=False,
    )
```
